512 devices in a mesh: tm: 8 (over z_hi, core), row: 16 (over z_lo, x), col: 4 (over y).
Axes of the slice: x: 4, y: 4, z: 16 (z_hi: 4, z_lo: 4; z = z_hi * 4 + z_lo), core: 2. Of those that a mesh axis runs over, the one named last changes fastest.
Arguments:
- occ_orbitals: bfloat16 [4096, 2048], P(('col', 'row'), 'tm'), may hold values from -0.4375 to 0.4375
- empty_orbitals: bfloat16 [4096, 2048], P(('col', 'row'), 'tm'), may hold values from -0.4375 to 0.4375
- occ_rate: float32 [2048], replicated, may hold values from 0.05 to 4
- empty_rate: float32 [2048], replicated, may hold values from 0.05 to 4
- columns: bfloat16 [4096, 256], P(('col', 'row')), may hold values from -6 to 6
Outputs:
- screened_columns: float32 [4096, 16, 256], P(('col', 'row'), 'tm')
The draws below stay inside these ranges and needn't reach their ends.
All inputs are finite; a program needn't handle non-finite values.
Results may differ from the reference program's by a relative error of at most 0.018.
Values may be sent and summed in bfloat16 or wider, within the bound.
A program may use at most 64 MiB of HBM per device.

```python
import math
import jax
import jax.numpy as jnp
from jax import lax

NO = 2048
NE = 2048
NT = 16
NF = 16
NC = 256
ROWS_DEV = 64
R = 4096
N_ROW = 16
N_COL = 4


def block_levels(key, shape, split, low, high):
    gain = 1.0
    for dim, shards_of in split:
        draws = jax.random.uniform(jax.random.fold_in(jax.random.fold_in(key, 6), dim), (shards_of,), jnp.float32, low / len(split), high / len(split))
        gain = gain * jnp.repeat(jnp.exp(draws), shape[dim] // shards_of).reshape((-1,) + (1,) * (len(shape) - 1 - dim))
    return gain


def scatter_about(rng, extent, scale, bound, cuts=(), kind=jnp.bfloat16):
    entries = scale * jax.random.normal(rng, extent, jnp.float32)
    if cuts:
        entries = entries * block_levels(rng, extent, cuts, -0.22, 0.18)
    return jnp.clip(entries, -bound, bound).astype(kind)


def setup_inputs(seed: int = 0) -> dict:
    arg_keys = jax.random.split(jax.random.key(seed), 6)
    return {
        "occ_orbitals": scatter_about(arg_keys[0], (R, NO), ((0.3 * NO * (NO + R ** 0.5)) ** -0.25), 0.4375, ((0, 64), (1, 8))),
        "empty_orbitals": scatter_about(arg_keys[1], (R, NE), ((0.3 * NE * (NE + R ** 0.5)) ** -0.25), 0.4375, ((0, 64), (1, 8))),
        "occ_rate": jnp.clip(jnp.exp(jax.random.uniform(arg_keys[2], (NO,), jnp.float32, math.log(0.05), math.log(4.0))), 0.05, 4.0),
        "empty_rate": jnp.clip(jnp.exp(jax.random.uniform(arg_keys[3], (NE,), jnp.float32, math.log(0.05), math.log(4.0))), 0.05, 4.0),
        "columns": scatter_about(arg_keys[4], (R, NC), 1.0, 6.0, ((0, 64),)),
    }


damping = 0.3


def time_tables(count_times, count_freqs):
    moments = 0.25 * (jnp.arange(count_times).astype(jnp.float32) + 0.5)
    omegas = 0.4 * (jnp.arange(count_freqs).astype(jnp.float32) + 0.5)
    cosine = (0.5 * jnp.cos(omegas[:, None] * moments[None, :])).astype(jnp.bfloat16)
    return moments, cosine


def spectral_block(occ_rows, empty_rows, occ_orbitals, empty_orbitals, occ_rate, empty_rate, moments, cosine):
    occ_full = occ_orbitals.astype(jnp.float32)
    empty_full = empty_orbitals.astype(jnp.float32)

    def one_time(moment):
        scaled_occ = (occ_rows.astype(jnp.float32) * jnp.exp(-occ_rate * moment)[None, :]).astype(jnp.bfloat16)
        scaled_empty = (empty_rows.astype(jnp.float32) * jnp.exp(-empty_rate * moment)[None, :]).astype(jnp.bfloat16)
        green_occ = jnp.einsum("ro,co->rc", scaled_occ.astype(jnp.float32), occ_full, precision=lax.Precision.HIGHEST)
        green_empty = jnp.einsum("ro,co->rc", scaled_empty.astype(jnp.float32), empty_full, precision=lax.Precision.HIGHEST)
        return (-2.0 * green_occ * green_empty).astype(jnp.bfloat16)

    polar = lax.map(one_time, moments)
    spectral = jnp.einsum("kj,jrc->krc", cosine.astype(jnp.float32), polar.astype(jnp.float32), precision=lax.Precision.HIGHEST)
    return spectral.astype(jnp.bfloat16)


def reference(occ_orbitals, empty_orbitals, occ_rate, empty_rate, columns):
    moments, cosine = time_tables(NT, NF)
    rows_tile = R // N_ROW
    block_count = N_ROW
    indices = jnp.arange(block_count).astype(jnp.int32)
    columns_wide = columns.astype(jnp.float32)

    def first_pass(index):
        start = (index * rows_tile).astype(jnp.int32)
        occ_rows = lax.dynamic_slice_in_dim(occ_orbitals, start, rows_tile, 0)
        empty_rows = lax.dynamic_slice_in_dim(empty_orbitals, start, rows_tile, 0)
        spectral = spectral_block(occ_rows, empty_rows, occ_orbitals, empty_orbitals, occ_rate, empty_rate, moments, cosine)
        return jnp.einsum("frc,cn->frn", spectral.astype(jnp.float32), columns_wide, precision=lax.Precision.HIGHEST)

    first = lax.map(first_pass, indices)
    first = jnp.transpose(first, (1, 0, 2, 3)).reshape(NF, R, NC)
    middle = (columns_wide[None, :, :] + damping * first).astype(jnp.bfloat16)
    group_span = ROWS_DEV * N_ROW
    base = (jnp.arange(N_COL).astype(jnp.int32)[:, None] * group_span + jnp.arange(ROWS_DEV).astype(jnp.int32)[None, :]).reshape(-1)

    def second_pass(total, index):
        picks = (base + index * ROWS_DEV).astype(jnp.int32)
        occ_rows = jnp.take(occ_orbitals, picks, axis=0)
        empty_rows = jnp.take(empty_orbitals, picks, axis=0)
        spectral = spectral_block(occ_rows, empty_rows, occ_orbitals, empty_orbitals, occ_rate, empty_rate, moments, cosine)
        middle_rows = jnp.take(middle, picks, axis=1)
        term = jnp.einsum("frc,frn->cfn", spectral.astype(jnp.float32), middle_rows.astype(jnp.float32), precision=lax.Precision.HIGHEST)
        rounded = lax.optimization_barrier(term.astype(jnp.bfloat16))
        return total + rounded.astype(jnp.float32), None

    second, unused = lax.scan(second_pass, jnp.zeros((R, NF, NC), jnp.float32), indices)
    return columns_wide[:, None, :] + damping * second
```

```python
import jax
import jax.numpy as jnp
import numpy as np
from jax import lax
from jax.experimental import pallas as pl
from jax.experimental.pallas import tpu as pltpu
from jax.sharding import PartitionSpec as P

MESH = pl.DeviceIdType.MESH
F32 = jnp.float32
BF16 = jnp.bfloat16
NT = 16
NZ = 16
DAMP = 0.3


def transform_matrix():
    moments = (0.25 * (np.arange(NT) + 0.5)).astype(np.float32)
    omegas = (0.4 * (np.arange(NT) + 0.5)).astype(np.float32)
    cosine = (0.5 * np.cos(omegas[:, None] * moments[None, :])).astype(np.float32)
    order = np.array([2 * tm + e for e in range(2) for tm in range(8)])
    return jnp.asarray(np.kron(cosine[order], np.eye(16)), dtype=BF16)


def kernel(
    occ_ref, emp_ref, x_ref, orate_ref, erate_ref, kron_ref, out_ref,
    colbuf, rowbuf, pk, lhs, acc, pol, spec, xc, fs, f1r, f1s, f2r, mb, yo, ysend, yrecv, zsend, zrecv,
    zag_s, zag_r, zd_s, zd_r, r1_s, r1_r, ag_s, ag_r, rs_s, rs_r, yd_s, yd_r, zr_s, zr_r,
):
    tm, row, y = lax.axis_index("tm"), lax.axis_index("row"), lax.axis_index("col")
    c, zh = tm % 2, tm // 2
    zl, x = row // 4, row % 4
    z = zh * 4 + zl
    u = x * (1 - c) + y * c
    v = y * (1 - c) + x * c

    def at_z(step):
        other = (z + step + NZ) % NZ
        return ((other // 4) * 2 + c, (other % 4) * 4 + x, y)

    def u_peer(d):
        return (tm, zl * 4 + (x + d * (1 - c)) % 4, (y + d * c) % 4)

    def v_peer(d):
        return (tm, zl * 4 + (x + d * c) % 4, (y + d * (1 - c)) % 4)

    partner = (zh * 2 + 1 - c, row, y)

    def remote(src, dst, ss, rs, dev):
        return pltpu.make_async_remote_copy(
            src_ref=src, dst_ref=dst, send_sem=ss, recv_sem=rs, device_id=dev, device_id_type=MESH
        )

    sends = []

    colbuf[c, z, 0:64, :] = occ_ref[...].reshape(64, 256)
    colbuf[c, z, 64:80, :] = x_ref[pl.ds(zh * 2, 2)].reshape(16, 256)
    colbuf[c, z, 80:144, :] = emp_ref[...].reshape(64, 256)
    for t in range(8):
        pk[t, 0] = occ_ref[t]
        pk[t, 1] = emp_ref[t]
    rowbuf[u, v, tm, 0] = occ_ref[tm]
    rowbuf[u, v, tm, 1] = emp_ref[tm]

    barrier = pltpu.get_barrier_semaphore()
    peers = [((tm + d) % 8, row, y) for d in range(1, 8)] + [at_z(1), at_z(-1)]
    peers += [u_peer(d) for d in range(1, 4)] + [v_peer(d) for d in range(1, 4)]
    for peer in peers:
        pl.semaphore_signal(barrier, inc=1, device_id=peer, device_id_type=MESH)
    pl.semaphore_wait(barrier, len(peers))

    halves = (pl.ds(0, 80), pl.ds(80, 64))

    def ring_copy(direction, t, sub):
        owner = (z - t + NZ) % NZ if direction == 0 else (z + t) % NZ
        ref = colbuf.at[c, owner, halves[sub], :]
        return remote(
            ref, ref, zag_s.at[direction, t, sub], zag_r.at[direction, t, sub], at_z(1 if direction == 0 else -1)
        )

    def pass_across(k, owner, sub):
        ref = colbuf.at[c, owner, halves[sub], :]
        copy = remote(ref, ref, zd_s.at[k, sub], zd_r.at[k, sub], partner)
        copy.start()
        sends.append(copy)
        return copy

    steps = (8, 7)
    across = []
    rings = {}
    for sub in range(2):
        for direction in range(2):
            rings[direction, 0, sub] = ring_copy(direction, 0, sub)
            rings[direction, 0, sub].start()
    r1 = []
    for d in range(1, 8):
        to = (tm + d) % 8
        cd = to % 2
        slot = rowbuf.at[x * (1 - cd) + y * cd, y * (1 - cd) + x * cd, tm]
        r1.append(remote(pk.at[to], slot, r1_s.at[d], r1_r.at[d], (to, row, y)))
        r1[-1].start()
    for sub in range(2):
        across.append(pass_across(0, z, sub))

    def ring_step(t):
        for sub in range(2):
            for direction in range(2):
                if t >= steps[direction]:
                    continue
                rings[direction, t, sub].wait_recv()
                if t + 1 < steps[direction]:
                    rings[direction, t + 1, sub] = ring_copy(direction, t + 1, sub)
                    rings[direction, t + 1, sub].start()
                owner = (z - 1 - t + NZ) % NZ if direction == 0 else (z + 1 + t) % NZ
                across.append(pass_across(1 + direction * 8 + t, owner, sub))

    acc[...] = jnp.zeros_like(acc)
    ring_step(0)
    ring_step(1)
    for copy in r1:
        copy.wait_recv()
    own = rowbuf.at[u, v]
    ag1 = [remote(own, own, ag_s.at[0, d], ag_r.at[0, d], v_peer(d)) for d in range(1, 4)]
    for copy in ag1:
        copy.start()
    ring_step(2)
    ring_step(3)
    for copy in ag1:
        copy.wait_recv()
    line = rowbuf.at[u]
    ag2 = [remote(line, line, ag_s.at[1, d], ag_r.at[1, d], u_peer(d)) for d in range(1, 4)]
    for copy in ag2:
        copy.start()
    for t in range(4, 8):
        ring_step(t)
    for copy in ag2:
        copy.wait_recv()
    for copy in across:
        copy.wait_recv()

    moments = 0.25 * (lax.broadcasted_iota(jnp.int32, (NT, 256), 0).astype(F32) + 0.5)

    @pl.loop(0, 8)
    def _(k):
        for s, rate_ref in ((0, orate_ref), (1, erate_ref)):
            weights = jnp.exp(-rate_ref[pl.ds(k, 1), :] * moments)
            rows = rowbuf[:, :, k, s].astype(F32).reshape(128, 256)
            for j in range(NT):
                lhs[s, j * 128 : (j + 1) * 128, :] = (rows * weights[j : j + 1, :]).astype(BF16)
            cols = colbuf[k % 2, pl.ds((k // 2) * 4, 4), s * 80 : s * 80 + 64, :].reshape(256, 256)
            acc[s] += lax.dot_general(
                lhs[s], cols, (((1,), (1,)), ((), ())), preferred_element_type=F32
            )

    for j in range(NT):
        at = pl.ds(j * 128, 128)
        pol[j] = (-2.0 * acc[0, at, :] * acc[1, at, :]).astype(BF16)
    for g in range(8):
        at = slice(g * 16, g * 16 + 16)
        mixed = jnp.dot(kron_ref[...], pol[:, at, :].reshape(256, 256), preferred_element_type=F32)
        spec[:, at, :] = mixed.astype(BF16).reshape(16, 16, 256)

    for h in range(4):
        for l in range(4):
            xc[l * 64 + h * 16 : l * 64 + h * 16 + 16, :] = colbuf[c, h * 4 + l, 64:80, :]

    rs1, rs2, mg1, mg2 = {}, {}, {}, {}
    for e in range(2):
        for k in range(8):
            part = jnp.dot(spec[e * 8 + k], xc[...], preferred_element_type=F32)
            fs[e, :, :, k] = part.reshape(4, 4, 8, 256).astype(BF16)
        rs1[e] = [
            remote(fs.at[e, (u + d) % 4], f1r.at[e, d - 1], rs_s.at[e, 0, d], rs_r.at[e, 0, d], u_peer(d))
            for d in range(1, 4)
        ]
        for copy in rs1[e]:
            copy.start()
    for e in range(2):
        for copy in rs1[e]:
            copy.wait_recv()
        total = fs[e, u].astype(F32)
        for d in range(3):
            total = total + f1r[e, d].astype(F32)
        f1s[e] = total.astype(BF16)
        rs2[e] = [
            remote(f1s.at[e, (v + d) % 4], f2r.at[e, d - 1], rs_s.at[e, 1, d], rs_r.at[e, 1, d], v_peer(d))
            for d in range(1, 4)
        ]
        for copy in rs2[e]:
            copy.start()
    for e in range(2):
        for copy in rs2[e]:
            copy.wait_recv()
        total = f1s[e, v].astype(F32)
        for d in range(3):
            total = total + f2r[e, d].astype(F32)
        mb[e, u, v] = (x_ref[tm].astype(F32)[None] + DAMP * total).astype(BF16)
        ref = mb.at[e, u, v]
        mg1[e] = [remote(ref, ref, rs_s.at[e, 2, d], rs_r.at[e, 2, d], v_peer(d)) for d in range(1, 4)]
        for copy in mg1[e]:
            copy.start()
    for e in range(2):
        for copy in mg1[e]:
            copy.wait_recv()
        ref = mb.at[e, u]
        mg2[e] = [remote(ref, ref, rs_s.at[e, 3, d], rs_r.at[e, 3, d], u_peer(d)) for d in range(1, 4)]
        for copy in mg2[e]:
            copy.start()

    def second(e, k):
        mid = mb[e, :, :, k].astype(F32).reshape(128, 256).astype(BF16)
        return lax.dot_general(
            spec[e * 8 + k], mid, (((0,), (0,)), ((), ())), preferred_element_type=F32
        ).reshape(4, 64, 256)

    def target(direction, t):
        return (z + 8 - t) % NZ if direction == 0 else (z - 7 + t + NZ) % NZ

    zr = {}

    def forward(e, direction, t, value):
        zsend[e, direction, t] = value.astype(BF16)
        zr[e, direction, t] = remote(
            zsend.at[e, direction, t],
            zrecv.at[e, direction, t],
            zr_s.at[e, direction, t],
            zr_r.at[e, direction, t],
            at_z(1 if direction == 0 else -1),
        )
        zr[e, direction, t].start()

    yd = {}
    for e in range(2):
        for copy in mg2[e]:
            copy.wait_recv()
        for h in range(4):
            ysend[e, h * 4 : h * 4 + 4] = second(e, h * 2 + 1 - c).astype(BF16)
        yd[e] = remote(ysend.at[e], yrecv.at[e], yd_s.at[e], yd_r.at[e], partner)
        yd[e].start()
        for h in range(4):
            yo[e, h * 4 : h * 4 + 4] = second(e, h * 2 + c)
        yd[e].wait_recv()
        for direction in range(2):
            d = target(direction, 0)
            forward(e, direction, 0, yo[e, d] + yrecv[e, d].astype(F32))
    for t in range(1, 8):
        for e in range(2):
            for direction in range(2):
                if t >= steps[direction]:
                    continue
                zr[e, direction, t - 1].wait_recv()
                d = target(direction, t)
                forward(
                    e, direction, t,
                    yo[e, d] + yrecv[e, d].astype(F32) + zrecv[e, direction, t - 1].astype(F32),
                )
    for e in range(2):
        zr[e, 0, 7].wait_recv()
        zr[e, 1, 6].wait_recv()
        total = yo[e, z] + yrecv[e, z].astype(F32) + zrecv[e, 0, 7].astype(F32) + zrecv[e, 1, 6].astype(F32)
        out_ref[e] = x_ref[...].reshape(64, 256).astype(F32) + DAMP * total

    for copy in sends:
        copy.wait_send()
    for group in (rings, zr, yd):
        for copy in group.values():
            copy.wait_send()
    for copies in (r1, ag1, ag2, *rs1.values(), *rs2.values(), *mg1.values(), *mg2.values()):
        for copy in copies:
            copy.wait_send()


def shards(occ_orbitals, empty_orbitals, occ_rate, empty_rate, columns):
    vmem = pl.BlockSpec(memory_space=pltpu.VMEM)
    dma = pltpu.SemaphoreType.DMA
    out = pl.pallas_call(
        kernel,
        out_shape=jax.ShapeDtypeStruct((2, 64, 256), F32),
        in_specs=[vmem] * 6,
        out_specs=vmem,
        scratch_shapes=[
            pltpu.VMEM((2, 16, 144, 256), BF16),
            pltpu.VMEM((4, 4, 8, 2, 8, 256), BF16),
            pltpu.VMEM((8, 2, 8, 256), BF16),
            pltpu.VMEM((2, 2048, 256), BF16),
            pltpu.VMEM((2, 2048, 256), F32),
            pltpu.VMEM((16, 128, 256), BF16),
            pltpu.VMEM((16, 128, 256), BF16),
            pltpu.VMEM((256, 256), BF16),
            pltpu.VMEM((2, 4, 4, 8, 8, 256), BF16),
            pltpu.VMEM((2, 3, 4, 8, 8, 256), BF16),
            pltpu.VMEM((2, 4, 8, 8, 256), BF16),
            pltpu.VMEM((2, 3, 8, 8, 256), BF16),
            pltpu.VMEM((2, 4, 4, 8, 8, 256), BF16),
            pltpu.VMEM((2, 16, 64, 256), F32),
            pltpu.VMEM((2, 16, 64, 256), BF16),
            pltpu.VMEM((2, 16, 64, 256), BF16),
            pltpu.VMEM((2, 2, 8, 64, 256), BF16),
            pltpu.VMEM((2, 2, 8, 64, 256), BF16),
            dma((2, 8, 2)), dma((2, 8, 2)),
            dma((16, 2)), dma((16, 2)),
            dma((8,)), dma((8,)),
            dma((2, 4)), dma((2, 4)),
            dma((2, 4, 4)), dma((2, 4, 4)),
            dma((2,)), dma((2,)),
            dma((2, 2, 8)), dma((2, 2, 8)),
        ],
        compiler_params=pltpu.CompilerParams(
            collective_id=0, has_side_effects=True, vmem_limit_bytes=60 * 1024 * 1024
        ),
        name="screen",
    )(
        occ_orbitals.reshape(8, 8, 256),
        empty_orbitals.reshape(8, 8, 256),
        columns.reshape(8, 8, 256),
        occ_rate.reshape(8, 256),
        empty_rate.reshape(8, 256),
        transform_matrix(),
    )
    return jnp.transpose(out, (1, 0, 2))


def solution(mesh):
    placed = (P(("col", "row"), "tm"), P(("col", "row"), "tm"), P(), P(), P(("col", "row"), None))
    return jax.shard_map(
        shards, mesh=mesh, in_specs=placed, out_specs=P(("col", "row"), "tm", None), check_vma=False
    )
```

```python
import jax
import jax.numpy as jnp
import numpy as np
from jax import lax
from jax.experimental import pallas as pl
from jax.experimental.pallas import tpu as pltpu
from jax.sharding import PartitionSpec as P

MESH = pl.DeviceIdType.MESH
F32 = jnp.float32
BF16 = jnp.bfloat16
NT = 16
NZ = 16
DAMP = 0.3
PIECES = ((0, 80), (80, 64), (144, 64), (208, 64))
OFFSET = ((144, 208), (0, 80))
UP, DOWN = 0, 1


_open = []


def phase(name):
    pass


def transform_matrix():
    moments = (0.25 * (np.arange(NT) + 0.5)).astype(np.float32)
    omegas = (0.4 * (np.arange(NT) + 0.5)).astype(np.float32)
    cosine = (0.5 * np.cos(omegas[:, None] * moments[None, :])).astype(np.float32)
    order = np.array([4 * zh + 2 * c + e for c in range(2) for e in range(2) for zh in range(4)])
    return jnp.asarray(np.kron(cosine[order], np.eye(16)), dtype=BF16)


def kernel(
    occ_ref, emp_ref, x_ref, orate_ref, erate_ref, kron_ref, out_ref,
    colbuf, rowbuf, pk, lhs, acc, pol, spec, xc, fs, f1r, f1s, f2r, mb, yo, ysend, yrecv, yloc, zsend, zrecv,
    zag_s, zag_r, zd_s, zd_r, zo_s, zo_r, r1_s, r1_r, ag1_s, ag1_r, ag2_s, ag2_r, rd_s, rd_r,
    rs_s, rs_r, yd_s, yd_r, yl_s, yl_r, zr_s, zr_r,
):
    tm, row, y = lax.axis_index("tm"), lax.axis_index("row"), lax.axis_index("col")
    c, zh = tm % 2, tm // 2
    zl, x = row // 4, row % 4
    z = zh * 4 + zl
    u = x * (1 - c) + y * c
    v = y * (1 - c) + x * c

    def at_z(step, core):
        other = (z + step + NZ) % NZ
        return ((other // 4) * 2 + core, (other % 4) * 4 + x, y)

    def plane(t, dx, dy):
        return (t, zl * 4 + (x + dx) % 4, (y + dy) % 4)

    def u_peer(d):
        return plane(tm, d * (1 - c), d * c)

    def v_peer(d):
        return plane(tm, d * c, d * (1 - c))

    partner = (zh * 2 + 1 - c, row, y)

    def remote(src, dst, ss, rs, dev):
        return pltpu.make_async_remote_copy(
            src_ref=src, dst_ref=dst, send_sem=ss, recv_sem=rs, device_id=dev, device_id_type=MESH
        )

    for t in range(8):
        pk[t, 0] = occ_ref[t]
        pk[t, 1] = emp_ref[t]

    @pl.when(c == 1)
    def _():
        colbuf[z, 0:64, :] = occ_ref[...].reshape(64, 256)
        colbuf[z, 64:80, :] = x_ref[pl.ds(zh * 2, 2)].reshape(16, 256)
        colbuf[z, 80:144, :] = emp_ref[...].reshape(64, 256)

    @pl.when(c == 0)
    def _():
        colbuf[z, 144:208, :] = occ_ref[...].reshape(64, 256)
        colbuf[z, 208:272, :] = emp_ref[...].reshape(64, 256)
        for h in range(2):
            uh, vh = (x, y) if h == 0 else (y, x)
            rowbuf[h, uh, vh, tm, 0] = occ_ref[zh * 2 + h]
            rowbuf[h, uh, vh, tm, 1] = emp_ref[zh * 2 + h]

    phase("bar")
    barrier = pltpu.get_barrier_semaphore()
    peers = [((tm + d) % 8, row, y) for d in range(1, 8)]
    peers += [at_z(step, core) for step in (1, -1) for core in (0, 1)]
    peers += [u_peer(d) for d in range(1, 4)] + [v_peer(d) for d in range(1, 4)]
    for peer in peers:
        pl.semaphore_signal(barrier, inc=1, device_id=peer, device_id_type=MESH)
    pl.semaphore_wait(barrier, len(peers))

    def to_row_gatherer(d, h):
        to = (zh + d) % 4
        uh, vh = (x, y) if h == 0 else (y, x)
        return remote(
            pk.at[to * 2 + h], rowbuf.at[h, uh, vh, tm], r1_s.at[d, h], r1_r.at[d, c, h], (to * 2, row, y)
        )

    def steps(piece, direction):
        return 8 if (piece < 2) == (direction == UP) else 7

    def shard(owner, piece):
        start, size = PIECES[piece]
        return colbuf.at[owner, pl.ds(start, size), :]

    def ring_copy(direction, t, piece):
        ref = shard((z - t + NZ) % NZ if direction == UP else (z + t) % NZ, piece)
        to = at_z(1 if direction == UP else -1, 1)
        return remote(ref, ref, zag_s.at[direction, t, piece], zag_r.at[direction, t, piece], to)

    def hand_over(direction, t, piece):
        ref = shard((z - 1 - t + NZ) % NZ if direction == UP else (z + 1 + t) % NZ, piece)
        return remote(ref, ref, zd_s.at[direction, t, piece], zd_r.at[direction, t, piece], partner)

    def own_over(piece):
        ref = shard(z, piece)
        return remote(ref, ref, zo_s.at[piece], zo_r.at[piece], partner)

    def row_over(uo, vo, i):
        ref = rowbuf.at[1, uo, vo]
        return remote(ref, ref, rd_s.at[i], rd_r.at[i], partner)

    acc[...] = jnp.zeros_like(acc)

    @pl.when(c == 1)
    def _():
        phase("issue")
        r1 = [to_row_gatherer(d, h) for d in range(4) for h in range(2)]
        started = []

        def start(copy):
            copy.start()
            started.append(copy)

        for copy in r1[2:]:
            start(copy)
        for piece in range(2):
            for direction in (UP, DOWN):
                start(ring_copy(direction, 0, piece))
        for copy in r1[:2]:
            start(copy)
        for piece in range(2):
            start(own_over(piece))
        for piece in range(2, 4):
            own_over(piece).wait_recv()
            for direction in (UP, DOWN):
                start(ring_copy(direction, 0, piece))
        for t in range(8):
            phase(f"z{t}")
            for piece in range(4):
                for direction in (UP, DOWN):
                    if t >= steps(piece, direction):
                        continue
                    ring_copy(direction, t, piece).wait_recv()
                    if t + 1 < steps(piece, direction):
                        start(ring_copy(direction, t + 1, piece))
                    start(hand_over(direction, t, piece))
        phase("roww")
        for i in range(16):
            row_over(0, 0, i).wait_recv()
        phase("sendw")
        for copy in started:
            copy.wait_send()

    @pl.when(c == 0)
    def _():
        phase("issue")
        started = []

        def start(copy):
            copy.start()
            started.append(copy)

        for piece in range(2, 4):
            start(own_over(piece))
        for d in range(1, 4):
            for h in range(2):
                start(to_row_gatherer(d, h))

        def first_stage(h, d):
            ref = rowbuf.at[h, x, y] if h == 0 else rowbuf.at[h, y, x]
            return remote(ref, ref, ag1_s.at[h, d], ag1_r.at[h, d], plane(tm, d * h, d * (1 - h)))

        def second_stage(h, d, back):
            uo, vo = (x, (y - back + 4) % 4) if h == 0 else (y, (x - back + 4) % 4)
            ref = rowbuf.at[h, uo, vo]
            return remote(ref, ref, ag2_s.at[h, d, back], ag2_r.at[h, d, back], plane(tm, d * (1 - h), d * h))

        def rows_over(d, back):
            start(row_over((y - d + 4) % 4, (x - back + 4) % 4, d * 4 + back))

        phase("r1w")
        for h in range(2):
            for core in range(2):
                for d in range(4):
                    if d or core:
                        ref = rowbuf.at[h, 0, 0, 0]
                        remote(ref, ref, r1_s.at[d, h], r1_r.at[d, core, h], partner).wait_recv()
        for h in range(2):
            for d in (2, 1, 3):
                start(first_stage(h, d))
            for d in (2, 1, 3):
                start(second_stage(h, d, 0))
        rows_over(0, 0)
        for back in (1, 3, 2):
            for h in range(2):
                phase(f"ag1w{back}{h}")
                first_stage(h, back).wait_recv()
                for d in (2, 1, 3):
                    start(second_stage(h, d, back))
            rows_over(0, back)
        for back in (0, 1, 3, 2):
            for d in (1, 3, 2):
                for h in (1, 0):
                    phase(f"ag2w{back}{d}{h}")
                    second_stage(h, d, back).wait_recv()
                    if h == 1:
                        rows_over(d, back)
        phase("colw")
        for piece in range(2):
            own_over(piece).wait_recv()
        for t in range(8):
            for piece in range(4):
                for direction in (UP, DOWN):
                    if t < steps(piece, direction):
                        hand_over(direction, t, piece).wait_recv()
        phase("sendw")
        for copy in started:
            copy.wait_send()

    phase("green")
    moments = 0.25 * (lax.broadcasted_iota(jnp.int32, (NT, 128), 0).astype(F32) + 0.5)

    @pl.loop(0, 4)
    def _(b):
        for s, rate_ref in ((0, orate_ref), (1, erate_ref)):
            cols = []
            for k in range(2):
                at = (b * 2 + k) * 2
                weights = jnp.concatenate(
                    [jnp.exp(-rate_ref[pl.ds(at + i, 1), :] * moments) for i in range(2)], axis=1
                )
                rows = rowbuf[c, :, :, b * 2 + k, s].astype(F32).reshape(128, 256)
                for j in range(NT):
                    lhs[s, j * 128 : (j + 1) * 128, k * 256 : (k + 1) * 256] = (
                        rows * weights[j : j + 1, :]
                    ).astype(BF16)
                cols.append(colbuf[pl.ds(b * 4, 4), OFFSET[k][s] : OFFSET[k][s] + 64, :].reshape(256, 256))
            acc[s] += lax.dot_general(
                lhs[s], jnp.concatenate(cols, axis=1), (((1,), (1,)), ((), ())), preferred_element_type=F32
            )

    phase("pol")
    for j in range(NT):
        at = pl.ds(j * 128, 128)
        pol[j] = (-2.0 * acc[0, at, :] * acc[1, at, :]).astype(BF16)
    phase("trans")
    for g in range(8):
        at = slice(g * 16, g * 16 + 16)
        mixed = jnp.dot(kron_ref[...], pol[:, at, :].reshape(256, 256), preferred_element_type=F32)
        spec[:, at, :] = mixed.astype(BF16).reshape(16, 16, 256)
    for h in range(4):
        for i in range(4):
            xc[i * 64 + h * 16 : i * 64 + h * 16 + 16, :] = colbuf[h * 4 + i, 64:80, :]

    def to_sum_u(q, d):
        return remote(fs.at[q, (u + d) % 4], f1r.at[q, d - 1], rs_s.at[q, 0, d], rs_r.at[q, 0, d], u_peer(d))

    def to_sum_v(q, d):
        return remote(f1s.at[q, (v + d) % 4], f2r.at[q, d - 1], rs_s.at[q, 1, d], rs_r.at[q, 1, d], v_peer(d))

    def gather_v(q, d):
        ref = mb.at[q, u, v]
        return remote(ref, ref, rs_s.at[q, 2, d], rs_r.at[q, 2, d], v_peer(d))

    def gather_u(q, d):
        ref = mb.at[q, u]
        return remote(ref, ref, rs_s.at[q, 3, d], rs_r.at[q, 3, d], u_peer(d))

    def all_three(make, q, started):
        for d in (2, 1, 3):
            copy = make(q, d)
            copy.start()
            started.append(copy)

    def arrived(make, q):
        for d in (1, 3, 2):
            make(q, d).wait_recv()

    first_sends = []
    for q in range(4):
        phase(f"first{q}")
        for k in range(4):
            part = jnp.dot(spec[q * 4 + k], xc[...], preferred_element_type=F32)
            fs[q, :, :, k] = part.reshape(4, 4, 8, 256).astype(BF16)
        all_three(to_sum_u, q, first_sends)

    def sum_u(q, started):
        phase(f"rs1w{q}")
        arrived(to_sum_u, q)
        phase(f"rs1c{q}")
        total = fs[q, u].astype(F32)
        for d in range(3):
            total = total + f1r[q, d].astype(F32)
        f1s[q] = total.astype(BF16)
        all_three(to_sum_v, q, started)

    def sum_v(q, started):
        phase(f"rs2w{q}")
        arrived(to_sum_v, q)
        phase(f"rs2c{q}")
        total = f1s[q, v].astype(F32)
        for d in range(3):
            total = total + f2r[q, d].astype(F32)
        mb[q, u, v] = (x_ref[tm].astype(F32)[None] + DAMP * total).astype(BF16)
        all_three(gather_v, q, started)

    def spread_u(q, started):
        phase(f"mg1w{q}")
        arrived(gather_v, q)
        all_three(gather_u, q, started)

    def second(q, k):
        mid = mb[q, :, :, k].astype(F32).reshape(128, 256).astype(BF16)
        return lax.dot_general(
            spec[q * 4 + k], mid, (((0,), (0,)), ((), ())), preferred_element_type=F32
        ).reshape(4, 64, 256)

    def pass_partials(q):
        return remote(ysend.at[q], yrecv.at[q], yd_s.at[q], yd_r.at[q], partner)

    def pass_local(q):
        return remote(ysend.at[q, z], yloc.at[q], yl_s.at[q], yl_r.at[q], partner)

    def sum_steps(q, direction):
        return 8 if (q < 2) == (direction == UP) else 7

    def ring_sum(q, direction, t):
        last = t + 1 == sum_steps(q, direction)
        return remote(
            zsend.at[q, direction, t],
            zrecv.at[q, direction, t],
            zr_s.at[q, direction, t],
            zr_r.at[q, direction, t],
            at_z(1 if direction == UP else -1, 0 if last and q < 2 else 1),
        )

    def finish(q, local):
        up, down = sum_steps(q, UP) - 1, sum_steps(q, DOWN) - 1
        ring_sum(q, UP, up).wait_recv()
        ring_sum(q, DOWN, down).wait_recv()
        total = local + zrecv[q, UP, up].astype(F32) + zrecv[q, DOWN, down].astype(F32)
        out_ref[q % 2] = x_ref[...].reshape(64, 256).astype(F32) + DAMP * total

    def events():
        listed = []
        for q in range(4):
            late = 1.4 * q
            listed += [(4.0 + late, sum_u, q), (6.9 + late, sum_v, q), (9.8 + late, spread_u, q)]
        return listed

    @pl.when(c == 1)
    def _():
        started = []

        def multiply(q, started):
            phase(f"mg2w{q}")
            arrived(gather_u, q)
            phase(f"mg2c{q}")
            for k in range(4):
                part = second(q, k)
                yo[q, k * 4 : k * 4 + 4] = part
            if q < 2:
                ysend[q, z] = yo[q, z].astype(BF16)
                copy = pass_local(q)
                copy.start()
                started.append(copy)

        def ring_step(q, started, t):
            phase(f"zr{t}{q}")
            if t == 0:
                pass_partials(q).wait_recv()
            for direction in (UP, DOWN):
                if t >= sum_steps(q, direction):
                    continue
                d = (
                    (z + sum_steps(q, UP) - t) % NZ
                    if direction == UP
                    else (z - sum_steps(q, DOWN) + t + NZ) % NZ
                )
                value = yo[q, d] + yrecv[q, d].astype(F32)
                if t:
                    ring_sum(q, direction, t - 1).wait_recv()
                    value = value + zrecv[q, direction, t - 1].astype(F32)
                zsend[q, direction, t] = value.astype(BF16)
                copy = ring_sum(q, direction, t)
                copy.start()
                started.append(copy)

        listed = [(at, act, q, ()) for at, act, q in events()]
        for q in range(4):
            late = 1.4 * q
            listed.append((13.8 + late, multiply, q, ()))
            for t in range(8):
                listed.append((15.8 + late + 2.1 * t, ring_step, q, (t,)))
        for _, act, q, more in sorted(listed, key=lambda item: item[0]):
            act(q, started, *more)
        for q in (2, 3):
            phase(f"fin{q}")
            finish(q, yo[q, z] + yrecv[q, z].astype(F32))
        phase("sendw2")
        for copy in started + first_sends:
            copy.wait_send()

    @pl.when(c == 0)
    def _():
        started = []

        def multiply(q, started):
            phase(f"mg2w{q}")
            arrived(gather_u, q)
            phase(f"mg2c{q}")
            for k in range(4):
                ysend[q, k * 4 : k * 4 + 4] = second(q, k).astype(BF16)
            copy = pass_partials(q)
            copy.start()
            started.append(copy)

        listed = events() + [(13.8 + 1.4 * q, multiply, q) for q in range(4)]
        for _, act, q in sorted(listed, key=lambda item: item[0]):
            act(q, started)
        for q in (0, 1):
            phase(f"fin{q}")
            pass_local(q).wait_recv()
            finish(q, ysend[q, z].astype(F32) + yloc[q].astype(F32))
        phase("sendw2")
        for copy in started + first_sends:
            copy.wait_send()

    phase(None)


def shards(occ_orbitals, empty_orbitals, occ_rate, empty_rate, columns):
    vmem = pl.BlockSpec(memory_space=pltpu.VMEM)
    dma = pltpu.SemaphoreType.DMA

    def pair(*shape):
        return [dma(shape), dma(shape)]

    out = pl.pallas_call(
        kernel,
        out_shape=jax.ShapeDtypeStruct((2, 64, 256), F32),
        in_specs=[vmem] * 6,
        out_specs=vmem,
        scratch_shapes=[
            pltpu.VMEM((16, 272, 256), BF16),
            pltpu.VMEM((2, 4, 4, 8, 2, 8, 256), BF16),
            pltpu.VMEM((8, 2, 8, 256), BF16),
            pltpu.VMEM((2, 2048, 512), BF16),
            pltpu.VMEM((2, 2048, 256), F32),
            pltpu.VMEM((16, 128, 256), BF16),
            pltpu.VMEM((16, 128, 256), BF16),
            pltpu.VMEM((256, 256), BF16),
            pltpu.VMEM((4, 4, 4, 4, 8, 256), BF16),
            pltpu.VMEM((4, 3, 4, 4, 8, 256), BF16),
            pltpu.VMEM((4, 4, 4, 8, 256), BF16),
            pltpu.VMEM((4, 3, 4, 8, 256), BF16),
            pltpu.VMEM((4, 4, 4, 4, 8, 256), BF16),
            pltpu.VMEM((4, 16, 64, 256), F32),
            pltpu.VMEM((4, 16, 64, 256), BF16),
            pltpu.VMEM((4, 16, 64, 256), BF16),
            pltpu.VMEM((2, 64, 256), BF16),
            pltpu.VMEM((4, 2, 8, 64, 256), BF16),
            pltpu.VMEM((4, 2, 8, 64, 256), BF16),
            *pair(2, 8, 4),
            *pair(2, 8, 4),
            *pair(4),
            dma((4, 2)), dma((4, 2, 2)),
            *pair(2, 4),
            *pair(2, 4, 4),
            *pair(16),
            *pair(4, 4, 4),
            *pair(4),
            *pair(2),
            *pair(4, 2, 8),
        ],
        compiler_params=pltpu.CompilerParams(
            collective_id=0, has_side_effects=True, vmem_limit_bytes=60 * 1024 * 1024
        ),
        name="screen",
    )(
        occ_orbitals.reshape(8, 8, 256),
        empty_orbitals.reshape(8, 8, 256),
        columns.reshape(8, 8, 256),
        occ_rate.reshape(16, 128),
        empty_rate.reshape(16, 128),
        transform_matrix(),
    )
    return jnp.transpose(out, (1, 0, 2))


def solution(mesh):
    placed = (P(("col", "row"), "tm"), P(("col", "row"), "tm"), P(), P(), P(("col", "row"), None))
    return jax.shard_map(
        shards, mesh=mesh, in_specs=placed, out_specs=P(("col", "row"), "tm", None), check_vma=False
    )
```

```python
import jax
import jax.numpy as jnp
import numpy as np
from jax import lax
from jax.experimental import pallas as pl
from jax.experimental.pallas import tpu as pltpu
from jax.sharding import PartitionSpec as P

MESH = pl.DeviceIdType.MESH
F32 = jnp.float32
BF16 = jnp.bfloat16
NT = 16
NZ = 16
DAMP = 0.3
PIECES = ((0, 10), (10, 8), (18, 8), (26, 8))
OFFSET = ((18, 26), (0, 10))
UP, DOWN = 0, 1


_open = []


def phase(name):
    pass


def transform_matrix():
    moments = (0.25 * (np.arange(NT) + 0.5)).astype(np.float32)
    omegas = (0.4 * (np.arange(NT) + 0.5)).astype(np.float32)
    cosine = (0.5 * np.cos(omegas[:, None] * moments[None, :])).astype(np.float32)
    order = np.array([4 * zh + 2 * c + e for c in range(2) for e in range(2) for zh in range(4)])
    return jnp.asarray(np.kron(cosine[order], np.eye(16)), dtype=BF16)


def kernel(
    occ_in, emp_in, x_in, orate_in, erate_in, kron_in, out_ref,
    x_ref, orate_ref, erate_ref, kron_ref,
    colbuf, rowbuf, pk, lhs, acc, pol, spec, xc, fs, f1r, f1s, f2r, mb, yo, ysend, yrecv, yloc, zsend, zrecv,
    in_s, zag_r, zd_r, zo_r, r1_r, ag1_r, ag2_r, rd_r, gs, rs_r, rs_s, yd_r, yl_r, ys, zr_r, zr_s,
):
    tm, row, y = lax.axis_index("tm"), lax.axis_index("row"), lax.axis_index("col")
    c, zh = tm % 2, tm // 2
    zl, x = row // 4, row % 4
    z = zh * 4 + zl
    u = x * (1 - c) + y * c
    v = y * (1 - c) + x * c

    def at_z(step, core):
        other = (z + step + NZ) % NZ
        return ((other // 4) * 2 + core, (other % 4) * 4 + x, y)

    def plane(t, dx, dy):
        return (t, zl * 4 + (x + dx) % 4, (y + dy) % 4)

    def u_peer(d):
        return plane(tm, d * (1 - c), d * c)

    def v_peer(d):
        return plane(tm, d * c, d * (1 - c))

    partner = (zh * 2 + 1 - c, row, y)

    def remote(src, dst, ss, rs, dev):
        return pltpu.make_async_remote_copy(
            src_ref=src, dst_ref=dst, send_sem=ss, recv_sem=rs, device_id=dev, device_id_type=MESH
        )

    rows_of = [(x, y), (y, x)]
    far = (zh + 2) % 4
    late = [
        pltpu.make_async_copy(src, dst, in_s.at[i])
        for i, (src, dst) in enumerate(
            ((x_in, x_ref), (orate_in, orate_ref), (erate_in, erate_ref), (kron_in, kron_ref))
        )
    ]
    early = []
    for s, src in enumerate((occ_in, emp_in)):
        early.append((src, colbuf.at[z, pl.ds(OFFSET[0][s] * (1 - c) + OFFSET[1][s] * c, 8)]))
        for h in range(2):
            early.append((src.at[far * 2 + h], pk.at[h, s]))
            early.append((src.at[zh * 2 + h], rowbuf.at[h, rows_of[h][0], rows_of[h][1], tm, s]))
    early = [pltpu.make_async_copy(src, dst, in_s.at[4]) for src, dst in early]
    own_x = pltpu.make_async_copy(x_in.at[pl.ds(zh * 2, 2)], colbuf.at[z, pl.ds(8, 2)], in_s.at[5])
    for copy in early:
        copy.start()

    @pl.when(c == 1)
    def _():
        own_x.start()

    for copy in late:
        copy.start()

    phase("bar")
    barrier = pltpu.get_barrier_semaphore()
    peers = [((tm + d) % 8, row, y) for d in range(1, 8)]
    peers += [at_z(step, core) for step in (1, -1) for core in (0, 1)]
    peers += [u_peer(d) for d in range(1, 4)] + [v_peer(d) for d in range(1, 4)]
    for peer in peers:
        pl.semaphore_signal(barrier, inc=1, device_id=peer, device_id_type=MESH)
    everything = ysend.at[0, pl.ds(0, 3)]
    pltpu.make_async_copy(everything, everything, in_s.at[4]).wait()

    @pl.when(c == 1)
    def _():
        own_x.wait()

    pl.semaphore_wait(barrier, len(peers))

    def received(ref, sem):
        remote(ref, ref, gs.at[0], sem, partner).wait_recv()

    def sent(ref, sem):
        remote(ref, ref, sem, zo_r.at[0], partner).wait_send()

    def to_row_gatherer(h):
        slot = rowbuf.at[h, rows_of[h][0], rows_of[h][1], tm]
        return remote(pk.at[h], slot, gs.at[0], r1_r, (far * 2, row, y))

    def steps(piece, direction):
        return 8 if (piece < 2) == (direction == UP) else 7

    def shard(owner, start, size):
        return colbuf.at[owner, pl.ds(start, size)]

    def ring_copy(direction, t, piece):
        ref = shard((z - t + NZ) % NZ if direction == UP else (z + t) % NZ, *PIECES[piece])
        to = at_z(1 if direction == UP else -1, 1)
        return remote(ref, ref, gs.at[1], zag_r.at[direction, t, piece], to)

    def hand_over(direction, t, piece):
        ref = shard((z - 1 - t + NZ) % NZ if direction == UP else (z + 1 + t) % NZ, *PIECES[piece])
        return remote(ref, ref, gs.at[2], zd_r.at[t // 4], partner)

    def own_over(start, size, i):
        ref = shard(z, start, size)
        return remote(ref, ref, gs.at[3], zo_r.at[i], partner)

    def rows_over(block):
        ref = rowbuf.at[1, :, :, pl.ds(block * 2, 2)]
        return remote(ref, ref, gs.at[4], rd_r, partner)

    acc[...] = jnp.zeros_like(acc)

    @pl.when(c == 1)
    def _():
        phase("issue")
        for h in range(2):
            to_row_gatherer(h).start()
        for piece in range(2):
            for direction in (UP, DOWN):
                ring_copy(direction, 0, piece).start()
        own_over(0, 18, 0).start()
        for piece in range(2, 4):
            own_over(*PIECES[piece], piece - 1).wait_recv()
            for direction in (UP, DOWN):
                ring_copy(direction, 0, piece).start()
        for t in range(8):
            phase(f"z{t}")
            for piece in range(4):
                for direction in (UP, DOWN):
                    if t >= steps(piece, direction):
                        continue
                    ring_copy(direction, t, piece).wait_recv()
                    if t + 1 < steps(piece, direction):
                        ring_copy(direction, t + 1, piece).start()
                    hand_over(direction, t, piece).start()
        phase("roww")
        received(rowbuf.at[1], rd_r)
        phase("sendw")
        sent(pk, gs.at[0])
        sent(colbuf.at[pl.ds(0, 15)], gs.at[1])
        sent(colbuf.at[pl.ds(0, 15)], gs.at[2])
        sent(colbuf.at[0, pl.ds(0, 18)], gs.at[3])

    @pl.when(c == 0)
    def _():
        phase("issue")
        for piece in range(2, 4):
            own_over(*PIECES[piece], piece - 1).start()
        for h in range(2):
            to_row_gatherer(h).start()

        def take_rows(owner, source):
            for s in range(2):
                for h in range(2):
                    slot = (h, rows_of[h][0], rows_of[h][1], (owner // 4) * 2 + source, s)
                    rowbuf[slot] = colbuf[owner, OFFSET[source][s] + zh * 2 + h]

        def first_stage(k):
            for d in (2, 1, 3):
                for h in range(2):
                    ref = rowbuf.at[h, rows_of[h][0], rows_of[h][1], pl.ds(((zh + k) % 4) * 2, 2)]
                    remote(ref, ref, gs.at[5], ag1_r.at[k], plane(tm, d * h, d * (1 - h))).start()

        def second_stage(k):
            phase(f"ag1w{k}")
            received(ysend.at[0, pl.ds(0, 3)], ag1_r.at[k])
            for back in range(4):
                for d in (2, 1, 3):
                    for h in range(2):
                        uo, vo = (x, (y - back + 4) % 4) if h == 0 else (y, (x - back + 4) % 4)
                        ref = rowbuf.at[h, uo, vo, pl.ds(((zh + k) % 4) * 2, 2)]
                        remote(ref, ref, gs.at[6], ag2_r.at[k], plane(tm, d * (1 - h), d * h)).start()

        def third_stage(k):
            phase(f"ag2w{k}")
            received(ysend.at[0, pl.ds(0, 12)], ag2_r.at[k])
            rows_over((zh + k) % 4).start()

        own_over(0, 18, 0).wait_recv()
        take_rows(z, 1)
        first_stage(0)
        second_stage(0)
        phase("r1w")
        received(ysend.at[0, 0], r1_r)
        first_stage(2)
        third_stage(0)
        second_stage(2)
        phase("z3w")
        received(colbuf.at[pl.ds(0, 8)], zd_r.at[0])
        for k in (1, 3):
            for source in range(2):
                take_rows((z + 4 * k) % NZ, source)
            first_stage(k)
        third_stage(2)
        for k in (1, 3):
            second_stage(k)
        for k in (1, 3):
            third_stage(k)
        phase("colw")
        received(colbuf.at[pl.ds(0, 7)], zd_r.at[1])
        phase("sendw")
        sent(pk, gs.at[0])
        sent(colbuf.at[0, pl.ds(0, 16)], gs.at[3])
        sent(rowbuf.at[1], gs.at[4])
        sent(ysend.at[0, pl.ds(0, 12)], gs.at[5])
        sent(ysend.at[pl.ds(0, 3)], gs.at[6])

    phase("green")
    for copy in late:
        copy.wait()
    moments = 0.25 * (lax.broadcasted_iota(jnp.int32, (NT, 128), 0).astype(F32) + 0.5)

    @pl.loop(0, 4)
    def _(b):
        for s, rate_ref in ((0, orate_ref), (1, erate_ref)):
            cols = []
            for k in range(2):
                at = (b * 2 + k) * 2
                weights = jnp.concatenate(
                    [jnp.exp(-rate_ref[pl.ds(at + i, 1), :] * moments) for i in range(2)], axis=1
                )
                rows = rowbuf[c, :, :, b * 2 + k, s].astype(F32).reshape(128, 256)
                for j in range(NT):
                    lhs[s, j * 128 : (j + 1) * 128, k * 256 : (k + 1) * 256] = (
                        rows * weights[j : j + 1, :]
                    ).astype(BF16)
                cols.append(colbuf[pl.ds(b * 4, 4), OFFSET[k][s] : OFFSET[k][s] + 8].reshape(256, 256))
            acc[s] += lax.dot_general(
                lhs[s], jnp.concatenate(cols, axis=1), (((1,), (1,)), ((), ())), preferred_element_type=F32
            )

    phase("pol")
    for j in range(NT):
        at = pl.ds(j * 128, 128)
        pol[j] = (-2.0 * acc[0, at, :] * acc[1, at, :]).astype(BF16)
    phase("trans")
    for g in range(8):
        at = slice(g * 16, g * 16 + 16)
        mixed = jnp.dot(kron_ref[...], pol[:, at, :].reshape(256, 256), preferred_element_type=F32)
        spec[:, at, :] = mixed.astype(BF16).reshape(16, 16, 256)
    for h in range(4):
        for i in range(4):
            xc[i * 64 + h * 16 : i * 64 + h * 16 + 16, :] = colbuf[h * 4 + i, 8:10].reshape(16, 256)

    def to_sum_u(q, d):
        return remote(fs.at[q, (u + d) % 4], f1r.at[q, d - 1], rs_s.at[0], rs_r.at[q, 0], u_peer(d))

    def to_sum_v(q, d):
        return remote(f1s.at[q, (v + d) % 4], f2r.at[q, d - 1], rs_s.at[1], rs_r.at[q, 1], v_peer(d))

    def gather_v(q, d):
        ref = mb.at[q, u, v]
        return remote(ref, ref, rs_s.at[2], rs_r.at[q, 2], v_peer(d))

    def gather_u(q, d):
        ref = mb.at[q, u]
        return remote(ref, ref, rs_s.at[3], rs_r.at[q, 3], u_peer(d))

    def all_three(make, q):
        for d in (2, 1, 3):
            make(q, d).start()

    for q in range(4):
        phase(f"first{q}")
        for k in range(4):
            part = jnp.dot(spec[q * 4 + k], xc[...], preferred_element_type=F32)
            fs[q, :, :, k] = part.reshape(4, 4, 8, 256).astype(BF16)
        all_three(to_sum_u, q)

    def sum_u(q):
        phase(f"rs1w{q}")
        received(f1r.at[q], rs_r.at[q, 0])
        phase(f"rs1c{q}")
        total = fs[q, u].astype(F32)
        for d in range(3):
            total = total + f1r[q, d].astype(F32)
        f1s[q] = total.astype(BF16)
        all_three(to_sum_v, q)

    def sum_v(q):
        phase(f"rs2w{q}")
        received(f2r.at[q], rs_r.at[q, 1])
        phase(f"rs2c{q}")
        total = f1s[q, v].astype(F32)
        for d in range(3):
            total = total + f2r[q, d].astype(F32)
        mb[q, u, v] = (x_ref[tm].astype(F32)[None] + DAMP * total).astype(BF16)
        all_three(gather_v, q)

    def spread_u(q):
        phase(f"mg1w{q}")
        received(mb.at[q, 0, pl.ds(0, 3)], rs_r.at[q, 2])
        all_three(gather_u, q)

    def second(q, k):
        mid = mb[q, :, :, k].astype(F32).reshape(128, 256).astype(BF16)
        return lax.dot_general(
            spec[q * 4 + k], mid, (((0,), (0,)), ((), ())), preferred_element_type=F32
        ).reshape(4, 64, 256)

    def pass_partials(q, k):
        at = pl.ds(k * 4, 4)
        return remote(ysend.at[q, at], yrecv.at[q, at], ys.at[0], yd_r.at[q], partner)

    def pass_local(q):
        return remote(ysend.at[q, z], yloc.at[q], ys.at[1], yl_r.at[q], partner)

    def sum_steps(q, direction):
        return 8 if (q < 2) == (direction == UP) else 7

    def ring_sum(q, direction, t):
        last = t + 1 == sum_steps(q, direction)
        return remote(
            zsend.at[q, direction, t],
            zrecv.at[q, direction, t],
            zr_s.at[q],
            zr_r.at[q, direction, t],
            at_z(1 if direction == UP else -1, 0 if last and q < 2 else 1),
        )

    def finish(q, local):
        up, down = sum_steps(q, UP) - 1, sum_steps(q, DOWN) - 1
        ring_sum(q, UP, up).wait_recv()
        ring_sum(q, DOWN, down).wait_recv()
        total = local + zrecv[q, UP, up].astype(F32) + zrecv[q, DOWN, down].astype(F32)
        out_ref[:, q % 2, :] = x_ref[...].reshape(64, 256).astype(F32) + DAMP * total

    def events():
        listed = []
        for q in range(4):
            late = 1.4 * q
            listed += [(4.0 + late, sum_u, q), (6.9 + late, sum_v, q), (9.8 + late, spread_u, q)]
        return listed

    @pl.when(c == 1)
    def _():
        def multiply(q):
            phase(f"mg2w{q}")
            received(mb.at[q, pl.ds(0, 3)], rs_r.at[q, 3])
            phase(f"mg2c{q}")
            for k in range(4):
                part = second(q, k)
                yo[q, k * 4 : k * 4 + 4] = part
            if q < 2:
                ysend[q, z] = yo[q, z].astype(BF16)
                pass_local(q).start()

        def ring_step(q, t):
            phase(f"zr{t}{q}")
            if t == 0:
                received(yrecv.at[q], yd_r.at[q])
            for direction in (UP, DOWN):
                if t >= sum_steps(q, direction):
                    continue
                d = (
                    (z + sum_steps(q, UP) - t) % NZ
                    if direction == UP
                    else (z - sum_steps(q, DOWN) + t + NZ) % NZ
                )
                value = yo[q, d] + yrecv[q, d].astype(F32)
                if t:
                    ring_sum(q, direction, t - 1).wait_recv()
                    value = value + zrecv[q, direction, t - 1].astype(F32)
                zsend[q, direction, t] = value.astype(BF16)
                ring_sum(q, direction, t).start()

        listed = [(at, act, q, ()) for at, act, q in events()]
        for q in range(4):
            late = 1.4 * q
            listed.append((13.8 + late, multiply, q, ()))
            for t in range(8):
                listed.append((15.8 + late + 2.4 * t, ring_step, q, (t,)))
        for _, act, q, more in sorted(listed, key=lambda item: item[0]):
            act(q, *more)
        for q in (2, 3):
            phase(f"fin{q}")
            finish(q, yo[q, z] + yrecv[q, z].astype(F32))
        phase("sendw2")
        for q in range(4):
            sent(ysend.at[0, pl.ds(0, 15)], zr_s.at[q])
        sent(yloc, ys.at[1])

    @pl.when(c == 0)
    def _():
        def multiply(q):
            phase(f"mg2w{q}")
            received(mb.at[q, pl.ds(0, 3)], rs_r.at[q, 3])
            phase(f"mg2c{q}")
            for k in range(4):
                ysend[q, k * 4 : k * 4 + 4] = second(q, k).astype(BF16)
                pass_partials(q, k).start()

        listed = events() + [(13.8 + 1.4 * q, multiply, q) for q in range(4)]
        for _, act, q in sorted(listed, key=lambda item: item[0]):
            act(q)
        for q in (0, 1):
            phase(f"fin{q}")
            pass_local(q).wait_recv()
            finish(q, ysend[q, z].astype(F32) + yloc[q].astype(F32))
        phase("sendw2")
        sent(ysend, ys.at[0])

    for i, ref in enumerate((fs.at[pl.ds(0, 3)], f2r, f2r, fs.at[pl.ds(0, 3)])):
        sent(ref, rs_s.at[i])

    phase(None)


def shards(occ_orbitals, empty_orbitals, occ_rate, empty_rate, columns):
    vmem = pl.BlockSpec(memory_space=pltpu.VMEM)
    dma = pltpu.SemaphoreType.DMA

    out = pl.pallas_call(
        kernel,
        out_shape=jax.ShapeDtypeStruct((64, 2, 256), F32),
        in_specs=[pl.BlockSpec(memory_space=pltpu.HBM)] * 6,
        out_specs=vmem,
        scratch_shapes=[
            pltpu.VMEM((8, 8, 256), BF16),
            pltpu.VMEM((16, 128), F32),
            pltpu.VMEM((16, 128), F32),
            pltpu.VMEM((256, 256), BF16),
            pltpu.VMEM((16, 34, 8, 256), BF16),
            pltpu.VMEM((2, 4, 4, 8, 2, 8, 256), BF16),
            pltpu.VMEM((2, 2, 8, 256), BF16),
            pltpu.VMEM((2, 2048, 512), BF16),
            pltpu.VMEM((2, 2048, 256), F32),
            pltpu.VMEM((16, 128, 256), BF16),
            pltpu.VMEM((16, 128, 256), BF16),
            pltpu.VMEM((256, 256), BF16),
            pltpu.VMEM((4, 4, 4, 4, 8, 256), BF16),
            pltpu.VMEM((4, 3, 4, 4, 8, 256), BF16),
            pltpu.VMEM((4, 4, 4, 8, 256), BF16),
            pltpu.VMEM((4, 3, 4, 8, 256), BF16),
            pltpu.VMEM((4, 4, 4, 4, 8, 256), BF16),
            pltpu.VMEM((4, 16, 64, 256), F32),
            pltpu.VMEM((4, 16, 64, 256), BF16),
            pltpu.VMEM((4, 16, 64, 256), BF16),
            pltpu.VMEM((2, 64, 256), BF16),
            pltpu.VMEM((4, 2, 8, 64, 256), BF16),
            pltpu.VMEM((4, 2, 8, 64, 256), BF16),
            dma((6,)),
            dma((2, 8, 4)),
            dma((2,)),
            dma((3,)),
            dma(()),
            dma((4,)),
            dma((4,)),
            dma(()),
            dma((7,)),
            dma((4, 4)), dma((4,)),
            dma((4,)), dma((2,)), dma((2,)),
            dma((4, 2, 8)), dma((4,)),
        ],
        compiler_params=pltpu.CompilerParams(
            collective_id=0, has_side_effects=True, vmem_limit_bytes=60 * 1024 * 1024
        ),
        name="screen",
    )(
        occ_orbitals.reshape(8, 8, 256),
        empty_orbitals.reshape(8, 8, 256),
        columns.reshape(8, 8, 256),
        occ_rate.reshape(16, 128),
        empty_rate.reshape(16, 128),
        transform_matrix(),
    )
    return out


def solution(mesh):
    placed = (P(("col", "row"), "tm"), P(("col", "row"), "tm"), P(), P(), P(("col", "row"), None))
    return jax.shard_map(
        shards, mesh=mesh, in_specs=placed, out_specs=P(("col", "row"), "tm", None), check_vma=False
    )
```

```python
import jax
import jax.numpy as jnp
import numpy as np
from jax import lax
from jax.experimental import pallas as pl
from jax.experimental.pallas import tpu as pltpu
from jax.sharding import PartitionSpec as P

MESH = pl.DeviceIdType.MESH
F32 = jnp.float32
BF16 = jnp.bfloat16
NT = 16
NZ = 16
DAMP = 0.3
PIECES = ((0, 10), (10, 8), (18, 8), (26, 8))
OFFSET = ((18, 26), (0, 10))
UP, DOWN = 0, 1
HOPS = (0, 1, 1, 1, 1, 1, 1, 1, 2)
SUM_HOPS = ((0, 1, 2, 1, 2, 1, 1, 1, 1), (0, 1, 2, 1, 2, 1, 2, 1, 2))


_open = []


def phase(name):
    pass


def transform_matrix():
    moments = (0.25 * (np.arange(NT) + 0.5)).astype(np.float32)
    omegas = (0.4 * (np.arange(NT) + 0.5)).astype(np.float32)
    cosine = (0.5 * np.cos(omegas[:, None] * moments[None, :])).astype(np.float32)
    order = np.array([4 * zh + 2 * c + e for c in range(2) for e in range(2) for zh in range(4)])
    return jnp.asarray(np.kron(cosine[order], np.eye(16)), dtype=BF16)


def kernel(
    occ_in, emp_in, x_in, orate_in, erate_in, kron_in, out_ref,
    x_ref, orate_ref, erate_ref, kron_ref,
    colbuf, rowbuf, pk, lhs, acc, pol, spec, xc, fs, f1r, f1s, f2r, mb, yo, ysend, yrecv, yloc, zsend, zrecv,
    in_s, zag_r, zd_r, zo_r, r1_r, ag1_r, ag2_r, rd_r, gs, rs_r, rs_s, yd_r, yl_r, ys, zr_r, zr_s,
):
    tm, row, y = lax.axis_index("tm"), lax.axis_index("row"), lax.axis_index("col")
    c, zh = tm % 2, tm // 2
    zl, x = row // 4, row % 4
    z = zh * 4 + zl
    u = x * (1 - c) + y * c
    v = y * (1 - c) + x * c

    def at_z(step, core):
        other = (z + step + NZ) % NZ
        return ((other // 4) * 2 + core, (other % 4) * 4 + x, y)

    def plane(t, dx, dy):
        return (t, zl * 4 + (x + dx) % 4, (y + dy) % 4)

    def u_peer(d):
        return plane(tm, d * (1 - c), d * c)

    def v_peer(d):
        return plane(tm, d * c, d * (1 - c))

    partner = (zh * 2 + 1 - c, row, y)

    def remote(src, dst, ss, rs, dev):
        return pltpu.make_async_remote_copy(
            src_ref=src, dst_ref=dst, send_sem=ss, recv_sem=rs, device_id=dev, device_id_type=MESH
        )

    rows_of = [(x, y), (y, x)]
    far = (zh + 2) % 4
    late = [
        pltpu.make_async_copy(src, dst, in_s.at[i])
        for i, (src, dst) in enumerate(
            ((x_in, x_ref), (orate_in, orate_ref), (erate_in, erate_ref), (kron_in, kron_ref))
        )
    ]
    early = []
    for s, src in enumerate((occ_in, emp_in)):
        early.append((src, colbuf.at[z, pl.ds(OFFSET[0][s] * (1 - c) + OFFSET[1][s] * c, 8)]))
        for h in range(2):
            early.append((src.at[far * 2 + h], pk.at[h, s]))
            early.append((src.at[zh * 2 + h], rowbuf.at[h, rows_of[h][0], rows_of[h][1], tm, s]))
    early = [pltpu.make_async_copy(src, dst, in_s.at[4]) for src, dst in early]
    own_x = pltpu.make_async_copy(x_in.at[pl.ds(zh * 2, 2)], colbuf.at[z, pl.ds(8, 2)], in_s.at[5])
    for copy in early:
        copy.start()

    @pl.when(c == 1)
    def _():
        own_x.start()

    for copy in late:
        copy.start()

    phase("bar")
    barrier = pltpu.get_barrier_semaphore()
    peers = [((tm + d) % 8, row, y) for d in range(1, 8)]
    peers += [at_z(step, core) for step in (1, -1, 2, -2) for core in (0, 1)]
    peers += [u_peer(d) for d in range(1, 4)] + [v_peer(d) for d in range(1, 4)]
    peers += [plane(tm + 1 - 2 * c, 0, d) for d in range(1, 4)]
    for peer in peers:
        pl.semaphore_signal(barrier, inc=1, device_id=peer, device_id_type=MESH)
    everything = ysend.at[0, pl.ds(0, 3)]
    pltpu.make_async_copy(everything, everything, in_s.at[4]).wait()

    @pl.when(c == 1)
    def _():
        own_x.wait()

    pl.semaphore_wait(barrier, len(peers))

    def received(ref, sem):
        remote(ref, ref, gs.at[0], sem, partner).wait_recv()

    def sent(ref, sem):
        remote(ref, ref, sem, zo_r.at[0], partner).wait_send()

    def to_row_gatherer(h):
        slot = rowbuf.at[h, rows_of[h][0], rows_of[h][1], tm]
        return remote(pk.at[h], slot, gs.at[0], r1_r, (far * 2, row, y))

    def steps(piece, direction):
        return 8 if (piece < 2) == (direction == UP) else 7

    def shard(owner, start, size):
        return colbuf.at[owner, pl.ds(start, size)]

    def ring_copy(direction, distance, piece):
        hop = HOPS[distance]
        sign = 1 if direction == UP else -1
        ref = shard((z - sign * (distance - hop) + NZ) % NZ, *PIECES[piece])
        return remote(ref, ref, gs.at[1], zag_r.at[direction, distance - 1, piece], at_z(sign * hop, 1))

    def pass_on(direction, reached, piece):
        for distance in (reached + 2, reached + 1):
            if distance <= steps(piece, direction) and HOPS[distance] == distance - reached:
                ring_copy(direction, distance, piece).start()

    def hand_over(direction, t, piece):
        ref = shard((z - 1 - t + NZ) % NZ if direction == UP else (z + 1 + t) % NZ, *PIECES[piece])
        return remote(ref, ref, gs.at[2], zd_r.at[t // 4], partner)

    def own_over(start, size, i):
        ref = shard(z, start, size)
        return remote(ref, ref, gs.at[3], zo_r.at[i], partner)

    def rows_over(block):
        ref = rowbuf.at[1, y, :, pl.ds(block * 2, 2)]
        return remote(ref, ref, gs.at[4], rd_r, partner)

    acc[...] = jnp.zeros_like(acc)

    @pl.when(c == 1)
    def _():
        phase("issue")
        for h in range(2):
            to_row_gatherer(h).start()
        for piece in range(2):
            for direction in (UP, DOWN):
                pass_on(direction, 0, piece)
        own_over(0, 18, 0).start()
        for piece in range(2, 4):
            own_over(*PIECES[piece], piece - 1).wait_recv()
            for direction in (UP, DOWN):
                pass_on(direction, 0, piece)
        for t in range(8):
            phase(f"z{t}")
            for piece in range(4):
                for direction in (UP, DOWN):
                    if t >= steps(piece, direction):
                        continue
                    ring_copy(direction, t + 1, piece).wait_recv()
                    pass_on(direction, t + 1, piece)
                    hand_over(direction, t, piece).start()
        phase("roww")
        received(rowbuf.at[1], rd_r)
        phase("sendw")
        sent(pk, gs.at[0])
        sent(colbuf.at[pl.ds(0, 15)], gs.at[1])
        sent(colbuf.at[pl.ds(0, 15)], gs.at[2])
        sent(colbuf.at[0, pl.ds(0, 18)], gs.at[3])

    @pl.when(c == 0)
    def _():
        phase("issue")
        for piece in range(2, 4):
            own_over(*PIECES[piece], piece - 1).start()
        for h in range(2):
            to_row_gatherer(h).start()

        def take_rows(owner, source):
            for s in range(2):
                for h in range(2):
                    slot = (h, rows_of[h][0], rows_of[h][1], (owner // 4) * 2 + source, s)
                    rowbuf[slot] = colbuf[owner, OFFSET[source][s] + zh * 2 + h]

        def first_stage(k):
            for d in (2, 1, 3):
                for h in range(2):
                    ref = rowbuf.at[h, rows_of[h][0], rows_of[h][1], pl.ds(((zh + k) % 4) * 2, 2)]
                    remote(ref, ref, gs.at[5], ag1_r.at[k], plane(tm, d * h, d * (1 - h))).start()

        def second_stage(k):
            phase(f"ag1w{k}")
            received(ysend.at[0, pl.ds(0, 3)], ag1_r.at[k])
            for back in range(4):
                for d in (2, 1, 3):
                    for h in range(2):
                        uo, vo = (x, (y - back + 4) % 4) if h == 0 else (y, (x - back + 4) % 4)
                        ref = rowbuf.at[h, uo, vo, pl.ds(((zh + k) % 4) * 2, 2)]
                        arrived = rd_r if h else ag2_r.at[k]
                        remote(ref, ref, gs.at[6], arrived, plane(tm + h, d * (1 - h), d * h)).start()
            rows_over((zh + k) % 4).start()

        def third_stage(k):
            phase(f"ag2w{k}")
            received(ysend.at[0, pl.ds(0, 6)], ag2_r.at[k])

        own_over(0, 18, 0).wait_recv()
        take_rows(z, 1)
        first_stage(0)
        second_stage(0)
        phase("r1w")
        received(ysend.at[0, 0], r1_r)
        first_stage(2)
        third_stage(0)
        second_stage(2)
        phase("z3w")
        received(colbuf.at[pl.ds(0, 8)], zd_r.at[0])
        for k in (1, 3):
            for source in range(2):
                take_rows((z + 4 * k) % NZ, source)
            first_stage(k)
        third_stage(2)
        for k in (1, 3):
            second_stage(k)
        for k in (1, 3):
            third_stage(k)
        phase("colw")
        received(colbuf.at[pl.ds(0, 7)], zd_r.at[1])
        phase("sendw")
        sent(pk, gs.at[0])
        sent(colbuf.at[0, pl.ds(0, 16)], gs.at[3])
        sent(rowbuf.at[1, 0], gs.at[4])
        sent(ysend.at[0, pl.ds(0, 12)], gs.at[5])
        sent(ysend.at[pl.ds(0, 3)], gs.at[6])

    phase("green")
    for copy in late:
        copy.wait()
    moments = 0.25 * (lax.broadcasted_iota(jnp.int32, (NT, 128), 0).astype(F32) + 0.5)

    @pl.loop(0, 2)
    def _(b):
        for s, rate_ref in ((0, orate_ref), (1, erate_ref)):
            cols = []
            for k in range(4):
                at = (b * 4 + k) * 2
                weights = jnp.concatenate(
                    [jnp.exp(-rate_ref[pl.ds(at + i, 1), :] * moments) for i in range(2)], axis=1
                )
                rows = rowbuf[c, :, :, b * 4 + k, s].astype(F32).reshape(128, 256)
                for j in range(NT):
                    lhs[s, j * 128 : (j + 1) * 128, k * 256 : (k + 1) * 256] = (
                        rows * weights[j : j + 1, :]
                    ).astype(BF16)
                first = OFFSET[k % 2][s]
                cols.append(colbuf[pl.ds(b * 8 + k // 2 * 4, 4), first : first + 8].reshape(256, 256))
            acc[s] += lax.dot_general(
                lhs[s], jnp.concatenate(cols, axis=1), (((1,), (1,)), ((), ())), preferred_element_type=F32
            )

    phase("pol")
    for j in range(NT):
        at = pl.ds(j * 128, 128)
        pol[j] = (-2.0 * acc[0, at, :] * acc[1, at, :]).astype(BF16)
    phase("trans")
    for g in range(8):
        at = slice(g * 16, g * 16 + 16)
        mixed = jnp.dot(kron_ref[...], pol[:, at, :].reshape(256, 256), preferred_element_type=F32)
        spec[:, at, :] = mixed.astype(BF16).reshape(16, 16, 256)
    for h in range(4):
        for i in range(4):
            xc[i * 64 + h * 16 : i * 64 + h * 16 + 16, :] = colbuf[h * 4 + i, 8:10].reshape(16, 256)

    def to_sum_u(q, d):
        return remote(fs.at[q, (u + d) % 4], f1r.at[q, d - 1], rs_s.at[0], rs_r.at[q, 0], u_peer(d))

    def to_sum_v(q, d):
        return remote(f1s.at[q, (v + d) % 4], f2r.at[q, d - 1], rs_s.at[1], rs_r.at[q, 1], v_peer(d))

    def gather_v(q, d):
        ref = mb.at[q, u, v]
        return remote(ref, ref, rs_s.at[2], rs_r.at[q, 2], v_peer(d))

    def gather_u(q, d):
        ref = mb.at[q, u]
        return remote(ref, ref, rs_s.at[3], rs_r.at[q, 3], u_peer(d))

    def all_three(make, q):
        for d in (2, 1, 3):
            make(q, d).start()

    for q in range(4):
        phase(f"first{q}")
        for k in range(4):
            part = jnp.dot(spec[q * 4 + k], xc[...], preferred_element_type=F32)
            fs[q, :, :, k] = part.reshape(4, 4, 8, 256).astype(BF16)
        all_three(to_sum_u, q)

    def sum_u(q):
        phase(f"rs1w{q}")
        received(f1r.at[q], rs_r.at[q, 0])
        phase(f"rs1c{q}")
        total = fs[q, u].astype(F32)
        for d in range(3):
            total = total + f1r[q, d].astype(F32)
        f1s[q] = total.astype(BF16)
        all_three(to_sum_v, q)

    def sum_v(q):
        phase(f"rs2w{q}")
        received(f2r.at[q], rs_r.at[q, 1])
        phase(f"rs2c{q}")
        total = f1s[q, v].astype(F32)
        for d in range(3):
            total = total + f2r[q, d].astype(F32)
        mb[q, u, v] = (x_ref[tm].astype(F32)[None] + DAMP * total).astype(BF16)
        all_three(gather_v, q)

    def spread_u(q):
        phase(f"mg1w{q}")
        received(mb.at[q, 0, pl.ds(0, 3)], rs_r.at[q, 2])
        all_three(gather_u, q)

    def second(q, k):
        mid = mb[q, :, :, k].astype(F32).reshape(128, 256).astype(BF16)
        return lax.dot_general(
            spec[q * 4 + k], mid, (((0,), (0,)), ((), ())), preferred_element_type=F32
        ).reshape(4, 64, 256)

    def pass_partials(q, k):
        at = pl.ds(k * 4, 4)
        return remote(ysend.at[q, at], yrecv.at[q, at], ys.at[0], yd_r.at[q], partner)

    def pass_local(q):
        return remote(ysend.at[q, z], yloc.at[q], ys.at[1], yl_r.at[q], partner)

    def sum_steps(q, direction):
        return 8 if (q < 2) == (direction == UP) else 7

    def sum_hop(q, distance):
        return SUM_HOPS[q // 2][distance]

    def sources(q, direction, left):
        return [d for d in range(8, 0, -1) if d <= sum_steps(q, direction) and d - sum_hop(q, d) == left]

    def ready(q, direction, left):
        after = [ready(q, direction, d) + 1.75 + 0.7 * sum_hop(q, d) for d in sources(q, direction, left)]
        return max(after, default=0.0)

    def ring_sum(q, direction, distance):
        hop = sum_hop(q, distance)
        sign = 1 if direction == UP else -1
        return remote(
            zsend.at[q, direction, distance - 1],
            zrecv.at[q, direction, distance - 1],
            zr_s.at[q],
            zr_r.at[q, direction, distance - 1],
            at_z(sign * hop, 0 if hop == distance and q < 2 else 1),
        )

    def ring_arrived(q, direction, left, value):
        for d in sources(q, direction, left):
            ring_sum(q, direction, d).wait_recv()
            value = value + zrecv[q, direction, d - 1].astype(F32)
        return value

    def finish(q, local):
        total = ring_arrived(q, DOWN, 0, ring_arrived(q, UP, 0, local))
        out_ref[:, q % 2, :] = x_ref[...].reshape(64, 256).astype(F32) + DAMP * total

    def events():
        listed = []
        for q in range(4):
            late = 1.4 * q
            listed += [(4.0 + late, sum_u, q), (6.9 + late, sum_v, q), (9.8 + late, spread_u, q)]
        return listed

    @pl.when(c == 1)
    def _():
        def multiply(q):
            phase(f"mg2w{q}")
            received(mb.at[q, pl.ds(0, 3)], rs_r.at[q, 3])
            phase(f"mg2c{q}")
            for k in range(4):
                part = second(q, k)
                yo[q, k * 4 : k * 4 + 4] = part
            if q < 2:
                ysend[q, z] = yo[q, z].astype(BF16)
                pass_local(q).start()

        def take_partials(q):
            phase(f"yw{q}")
            received(yrecv.at[q], yd_r.at[q])

        def ring_step(q, direction, distance):
            phase(f"zr{distance}{q}")
            sign = 1 if direction == UP else -1
            d = (z + sign * distance + NZ) % NZ
            value = ring_arrived(q, direction, distance, yo[q, d] + yrecv[q, d].astype(F32))
            zsend[q, direction, distance - 1] = value.astype(BF16)
            ring_sum(q, direction, distance).start()

        listed = [(at, act, q, ()) for at, act, q in events()]
        for q in range(4):
            late = 1.4 * q
            listed.append((13.8 + late, multiply, q, ()))
            listed.append((15.8 + late, take_partials, q, ()))
            for distance in range(8, 0, -1):
                for direction in (UP, DOWN):
                    if distance <= sum_steps(q, direction):
                        at = 15.8 + late + ready(q, direction, distance)
                        listed.append((at, ring_step, q, (direction, distance)))
        for _, act, q, more in sorted(listed, key=lambda item: item[0]):
            act(q, *more)
        for q in (2, 3):
            phase(f"fin{q}")
            finish(q, yo[q, z] + yrecv[q, z].astype(F32))
        phase("sendw2")
        for q in range(4):
            sent(ysend.at[0, pl.ds(0, 15)], zr_s.at[q])
        sent(yloc, ys.at[1])

    @pl.when(c == 0)
    def _():
        def multiply(q):
            phase(f"mg2w{q}")
            received(mb.at[q, pl.ds(0, 3)], rs_r.at[q, 3])
            phase(f"mg2c{q}")
            for k in range(4):
                ysend[q, k * 4 : k * 4 + 4] = second(q, k).astype(BF16)
                pass_partials(q, k).start()

        listed = events() + [(13.8 + 1.4 * q, multiply, q) for q in range(4)]
        for _, act, q in sorted(listed, key=lambda item: item[0]):
            act(q)
        for q in (0, 1):
            phase(f"fin{q}")
            pass_local(q).wait_recv()
            finish(q, ysend[q, z].astype(F32) + yloc[q].astype(F32))
        phase("sendw2")
        sent(ysend, ys.at[0])

    for i, ref in enumerate((fs.at[pl.ds(0, 3)], f2r, f2r, fs.at[pl.ds(0, 3)])):
        sent(ref, rs_s.at[i])

    phase(None)


def shards(occ_orbitals, empty_orbitals, occ_rate, empty_rate, columns):
    vmem = pl.BlockSpec(memory_space=pltpu.VMEM)
    dma = pltpu.SemaphoreType.DMA

    out = pl.pallas_call(
        kernel,
        out_shape=jax.ShapeDtypeStruct((64, 2, 256), F32),
        in_specs=[pl.BlockSpec(memory_space=pltpu.HBM)] * 6,
        out_specs=vmem,
        scratch_shapes=[
            pltpu.VMEM((8, 8, 256), BF16),
            pltpu.VMEM((16, 128), F32),
            pltpu.VMEM((16, 128), F32),
            pltpu.VMEM((256, 256), BF16),
            pltpu.VMEM((16, 34, 8, 256), BF16),
            pltpu.VMEM((2, 4, 4, 8, 2, 8, 256), BF16),
            pltpu.VMEM((2, 2, 8, 256), BF16),
            pltpu.VMEM((2, 2048, 1024), BF16),
            pltpu.VMEM((2, 2048, 256), F32),
            pltpu.VMEM((16, 128, 256), BF16),
            pltpu.VMEM((16, 128, 256), BF16),
            pltpu.VMEM((256, 256), BF16),
            pltpu.VMEM((4, 4, 4, 4, 8, 256), BF16),
            pltpu.VMEM((4, 3, 4, 4, 8, 256), BF16),
            pltpu.VMEM((4, 4, 4, 8, 256), BF16),
            pltpu.VMEM((4, 3, 4, 8, 256), BF16),
            pltpu.VMEM((4, 4, 4, 4, 8, 256), BF16),
            pltpu.VMEM((4, 16, 64, 256), F32),
            pltpu.VMEM((4, 16, 64, 256), BF16),
            pltpu.VMEM((4, 16, 64, 256), BF16),
            pltpu.VMEM((2, 64, 256), BF16),
            pltpu.VMEM((4, 2, 8, 64, 256), BF16),
            pltpu.VMEM((4, 2, 8, 64, 256), BF16),
            dma((6,)),
            dma((2, 8, 4)),
            dma((2,)),
            dma((3,)),
            dma(()),
            dma((4,)),
            dma((4,)),
            dma(()),
            dma((7,)),
            dma((4, 4)), dma((4,)),
            dma((4,)), dma((2,)), dma((2,)),
            dma((4, 2, 8)), dma((4,)),
        ],
        compiler_params=pltpu.CompilerParams(
            collective_id=0, has_side_effects=True, vmem_limit_bytes=48 * 1024 * 1024
        ),
        name="screen",
    )(
        *(
            pltpu.with_memory_space_constraint(a, pltpu.HBM)
            for a in (
                occ_orbitals.reshape(8, 8, 256),
                empty_orbitals.reshape(8, 8, 256),
                columns.reshape(8, 8, 256),
                occ_rate.reshape(16, 128),
                empty_rate.reshape(16, 128),
                transform_matrix(),
            )
        )
    )
    return out


def solution(mesh):
    placed = (P(("col", "row"), "tm"), P(("col", "row"), "tm"), P(), P(), P(("col", "row"), None))
    return jax.shard_map(
        shards, mesh=mesh, in_specs=placed, out_specs=P(("col", "row"), "tm", None), check_vma=False
    )
```

```python
import jax
import jax.numpy as jnp
import numpy as np
from jax import lax
from jax.experimental import pallas as pl
from jax.experimental.pallas import tpu as pltpu
from jax.sharding import PartitionSpec as P

MESH = pl.DeviceIdType.MESH
F32 = jnp.float32
BF16 = jnp.bfloat16
NT = 16
NZ = 16
DAMP = 0.3
PIECES = ((0, 10), (10, 8), (18, 8), (26, 8))
OFFSET = ((18, 26), (0, 10))
UP, DOWN = 0, 1
HOPS = (0, 1, 1, 1, 1, 1, 1, 1, 2)
SUM_HOPS = ((0, 1, 2, 1, 2, 1, 1, 1, 1), (0, 1, 2, 1, 2, 1, 2, 1, 2))


_open = []


def phase(name):
    pass


def transform_matrix():
    moments = (0.25 * (np.arange(NT) + 0.5)).astype(np.float32)
    omegas = (0.4 * (np.arange(NT) + 0.5)).astype(np.float32)
    cosine = (0.5 * np.cos(omegas[:, None] * moments[None, :])).astype(np.float32)
    order = np.array([4 * zh + 2 * c + e for c in range(2) for e in range(2) for zh in range(4)])
    return jnp.asarray(np.kron(cosine[order], np.eye(16)), dtype=BF16)


def kernel(
    occ_in, emp_in, x_in, orate_in, erate_in, kron_in, out_ref,
    x_ref, orate_ref, erate_ref, kron_ref,
    colbuf, rowbuf, pk, lhs, acc, pol, spec, xc, fs, f1r, f1s, f2r, mb, yo, ysend, yrecv, yloc, zsend, zrecv,
    in_s, zag_r, zd_r, zo_r, r1_r, ag1_r, ag2_r, rd_r, gs, rs_r, rs_s, yd_r, yl_r, ys, zr_r, zr_s,
):
    tm, row, y = lax.axis_index("tm"), lax.axis_index("row"), lax.axis_index("col")
    c, zh = tm % 2, tm // 2
    zl, x = row // 4, row % 4
    z = zh * 4 + zl
    u = x * (1 - c) + y * c
    v = y * (1 - c) + x * c

    def at_z(step, core):
        other = (z + step + NZ) % NZ
        return ((other // 4) * 2 + core, (other % 4) * 4 + x, y)

    def plane(t, dx, dy):
        return (t, zl * 4 + (x + dx) % 4, (y + dy) % 4)

    def u_peer(d):
        return plane(tm, d * (1 - c), d * c)

    def v_peer(d):
        return plane(tm, d * c, d * (1 - c))

    partner = (zh * 2 + 1 - c, row, y)

    def remote(src, dst, ss, rs, dev):
        return pltpu.make_async_remote_copy(
            src_ref=src, dst_ref=dst, send_sem=ss, recv_sem=rs, device_id=dev, device_id_type=MESH
        )

    rows_of = [(x, y), (y, x)]
    far = (zh + 2) % 4
    late = [
        pltpu.make_async_copy(src, dst, in_s.at[i])
        for i, (src, dst) in enumerate(
            ((x_in, x_ref), (orate_in, orate_ref), (erate_in, erate_ref), (kron_in, kron_ref))
        )
    ]
    early = []
    for s, src in enumerate((occ_in, emp_in)):
        early.append((src, colbuf.at[z, pl.ds(OFFSET[0][s] * (1 - c) + OFFSET[1][s] * c, 8)]))
        for h in range(2):
            early.append((src.at[far * 2 + h], pk.at[h, s]))
            early.append((src.at[zh * 2 + h], rowbuf.at[h, rows_of[h][0], rows_of[h][1], tm, s]))
    early = [pltpu.make_async_copy(src, dst, in_s.at[4]) for src, dst in early]
    own_x = pltpu.make_async_copy(x_in.at[pl.ds(zh * 2, 2)], colbuf.at[z, pl.ds(8, 2)], in_s.at[5])
    for copy in early:
        copy.start()

    @pl.when(c == 1)
    def _():
        own_x.start()

    for copy in late:
        copy.start()

    phase("bar")
    barrier = pltpu.get_barrier_semaphore()
    peers = [((tm + d) % 8, row, y) for d in range(1, 8)]
    peers += [at_z(step, core) for step in (1, -1, 2, -2) for core in (0, 1)]
    peers += [u_peer(d) for d in range(1, 4)] + [v_peer(d) for d in range(1, 4)]
    peers += [plane(tm + 1 - 2 * c, 0, d) for d in range(1, 4)]
    peers += [plane(tm + 1 - 2 * c, d, 0) for d in range(1, 4)]
    for peer in peers:
        pl.semaphore_signal(barrier, inc=1, device_id=peer, device_id_type=MESH)
    everything = ysend.at[0, pl.ds(0, 3)]
    pltpu.make_async_copy(everything, everything, in_s.at[4]).wait()

    @pl.when(c == 1)
    def _():
        own_x.wait()

    pl.semaphore_wait(barrier, len(peers))

    def received(ref, sem):
        remote(ref, ref, gs.at[0], sem, partner).wait_recv()

    def sent(ref, sem):
        remote(ref, ref, sem, zo_r.at[0], partner).wait_send()

    def to_row_gatherer(h):
        slot = rowbuf.at[h, rows_of[h][0], rows_of[h][1], tm]
        return remote(pk.at[h], slot, gs.at[0], r1_r, (far * 2, row, y))

    def steps(piece, direction):
        return 8 if (piece < 2) == (direction == UP) else 7

    def shard(owner, start, size):
        return colbuf.at[owner, pl.ds(start, size)]

    def ring_copy(direction, distance, piece):
        hop = HOPS[distance]
        sign = 1 if direction == UP else -1
        ref = shard((z - sign * (distance - hop) + NZ) % NZ, *PIECES[piece])
        return remote(ref, ref, gs.at[1], zag_r.at[direction, distance - 1, piece], at_z(sign * hop, 1))

    def pass_on(direction, reached, piece):
        for distance in (reached + 2, reached + 1):
            if distance <= steps(piece, direction) and HOPS[distance] == distance - reached:
                ring_copy(direction, distance, piece).start()

    def hand_over(direction, t, piece):
        ref = shard((z - 1 - t + NZ) % NZ if direction == UP else (z + 1 + t) % NZ, *PIECES[piece])
        return remote(ref, ref, gs.at[2], zd_r.at[t // 4], partner)

    def own_over(start, size, i):
        ref = shard(z, start, size)
        return remote(ref, ref, gs.at[3], zo_r.at[i], partner)

    def rows_over(block):
        ref = rowbuf.at[1, y, :, pl.ds(block * 2, 2)]
        return remote(ref, ref, gs.at[4], rd_r, partner)

    acc[...] = jnp.zeros_like(acc)

    @pl.when(c == 1)
    def _():
        phase("issue")
        for h in range(2):
            to_row_gatherer(h).start()
        for piece in range(2):
            for direction in (UP, DOWN):
                pass_on(direction, 0, piece)
        own_over(0, 18, 0).start()
        for piece in range(2, 4):
            own_over(*PIECES[piece], piece - 1).wait_recv()
            for direction in (UP, DOWN):
                pass_on(direction, 0, piece)
        for t in range(8):
            phase(f"z{t}")
            for piece in range(4):
                for direction in (UP, DOWN):
                    if t >= steps(piece, direction):
                        continue
                    ring_copy(direction, t + 1, piece).wait_recv()
                    pass_on(direction, t + 1, piece)
                    hand_over(direction, t, piece).start()
        phase("roww")
        received(rowbuf.at[1], rd_r)
        phase("sendw")
        sent(pk, gs.at[0])
        sent(colbuf.at[pl.ds(0, 15)], gs.at[1])
        sent(colbuf.at[pl.ds(0, 15)], gs.at[2])
        sent(colbuf.at[0, pl.ds(0, 18)], gs.at[3])

    @pl.when(c == 0)
    def _():
        phase("issue")
        for piece in range(2, 4):
            own_over(*PIECES[piece], piece - 1).start()
        for h in range(2):
            to_row_gatherer(h).start()

        def take_rows(owner, source):
            for s in range(2):
                for h in range(2):
                    slot = (h, rows_of[h][0], rows_of[h][1], (owner // 4) * 2 + source, s)
                    rowbuf[slot] = colbuf[owner, OFFSET[source][s] + zh * 2 + h]

        def first_stage(k):
            for d in (2, 1, 3):
                for h in range(2):
                    ref = rowbuf.at[h, rows_of[h][0], rows_of[h][1], pl.ds(((zh + k) % 4) * 2, 2)]
                    remote(ref, ref, gs.at[5], ag1_r.at[k], plane(tm, d * h, d * (1 - h))).start()

        def second_stage(k):
            phase(f"ag1w{k}")
            received(ysend.at[0, pl.ds(0, 3)], ag1_r.at[k])
            for back in range(4):
                for d in (2, 1, 3):
                    for h in range(2):
                        uo, vo = (x, (y - back + 4) % 4) if h == 0 else (y, (x - back + 4) % 4)
                        ref = rowbuf.at[h, uo, vo, pl.ds(((zh + k) % 4) * 2, 2)]
                        arrived = rd_r if h else ag2_r.at[k]
                        remote(ref, ref, gs.at[6], arrived, plane(tm + h, d * (1 - h), d * h)).start()
            rows_over((zh + k) % 4).start()

        def third_stage(k):
            phase(f"ag2w{k}")
            received(ysend.at[0, pl.ds(0, 6)], ag2_r.at[k])

        own_over(0, 18, 0).wait_recv()
        take_rows(z, 1)
        first_stage(0)
        second_stage(0)
        phase("r1w")
        received(ysend.at[0, 0], r1_r)
        first_stage(2)
        third_stage(0)
        second_stage(2)
        phase("z3w")
        received(colbuf.at[pl.ds(0, 8)], zd_r.at[0])
        for k in (1, 3):
            for source in range(2):
                take_rows((z + 4 * k) % NZ, source)
            first_stage(k)
        third_stage(2)
        for k in (1, 3):
            second_stage(k)
        for k in (1, 3):
            third_stage(k)
        phase("colw")
        received(colbuf.at[pl.ds(0, 7)], zd_r.at[1])
        phase("sendw")
        sent(pk, gs.at[0])
        sent(colbuf.at[0, pl.ds(0, 16)], gs.at[3])
        sent(rowbuf.at[1, 0], gs.at[4])
        sent(ysend.at[0, pl.ds(0, 12)], gs.at[5])
        sent(ysend.at[pl.ds(0, 3)], gs.at[6])

    phase("green")
    for copy in late:
        copy.wait()
    moments = 0.25 * (lax.broadcasted_iota(jnp.int32, (NT, 128), 0).astype(F32) + 0.5)

    @pl.loop(0, 2)
    def _(b):
        for s, rate_ref in ((0, orate_ref), (1, erate_ref)):
            cols = []
            for k in range(4):
                at = (b * 4 + k) * 2
                weights = jnp.concatenate(
                    [jnp.exp(-rate_ref[pl.ds(at + i, 1), :] * moments) for i in range(2)], axis=1
                )
                rows = rowbuf[c, :, :, b * 4 + k, s].astype(F32).reshape(128, 256)
                for j in range(NT):
                    lhs[s, j * 128 : (j + 1) * 128, k * 256 : (k + 1) * 256] = (
                        rows * weights[j : j + 1, :]
                    ).astype(BF16)
                first = OFFSET[k % 2][s]
                cols.append(colbuf[pl.ds(b * 8 + k // 2 * 4, 4), first : first + 8].reshape(256, 256))
            acc[s] += lax.dot_general(
                lhs[s], jnp.concatenate(cols, axis=1), (((1,), (1,)), ((), ())), preferred_element_type=F32
            )

    phase("pol")
    for j in range(NT):
        at = pl.ds(j * 128, 128)
        pol[j] = (-2.0 * acc[0, at, :] * acc[1, at, :]).astype(BF16)
    phase("trans")
    for g in range(8):
        at = slice(g * 16, g * 16 + 16)
        mixed = jnp.dot(kron_ref[...], pol[:, at, :].reshape(256, 256), preferred_element_type=F32)
        spec[:, at, :] = mixed.astype(BF16).reshape(16, 16, 256)
    for h in range(4):
        for i in range(4):
            xc[i * 64 + h * 16 : i * 64 + h * 16 + 16, :] = colbuf[h * 4 + i, 8:10].reshape(16, 256)

    def to_sum_u(q, d):
        to = plane(zh * 2 + 1, d * (1 - c), d * c)
        return remote(fs.at[q, (u + d) % 4], f1r.at[c, q, d], rs_s.at[0], rs_r.at[c, q, 0], to)

    def along_v(src, dst, stage, h, q, d):
        plane_v = plane(tm, d * h, d * (1 - h))
        remote(src, dst, rs_s.at[stage], rs_r.at[h, q, stage], plane_v).start()

    for q in range(4):
        phase(f"first{q}")
        for k in range(4):
            part = jnp.dot(spec[q * 4 + k], xc[...], preferred_element_type=F32)
            fs[q, :, :, k] = part.reshape(4, 4, 8, 256).astype(BF16)
        for d in (2, 1, 3):
            to_sum_u(q, d).start()

        @pl.when(c == 0)
        def _(q=q):
            to_sum_u(q, 0).start()

    def sum_u(q, h):
        phase(f"rs1w{q}{h}")
        received(f1r.at[1, q, pl.ds(1, 3)] if h else f1r.at[0, q], rs_r.at[h, q, 0])
        total = (fs[q, u] if h else f1r[0, q, 0]).astype(F32)
        for d in range(1, 4):
            total = total + f1r[h, q, d].astype(F32)
        f1s[h, q] = total.astype(BF16)
        for d in (2, 1, 3):
            along_v(f1s.at[h, q, (rows_of[h][1] + d) % 4], f2r.at[h, q, d - 1], 1, h, q, d)

    def sum_v(q, h):
        phase(f"rs2w{q}{h}")
        received(f2r.at[h, q], rs_r.at[h, q, 1])
        total = f1s[h, q, rows_of[h][1]].astype(F32)
        for d in range(3):
            total = total + f2r[h, q, d].astype(F32)
        mb[h, q, rows_of[h][0], rows_of[h][1]] = (
            x_ref[zh * 2 + h].astype(F32)[None] + DAMP * total
        ).astype(BF16)
        ref = mb.at[h, q, rows_of[h][0], rows_of[h][1]]
        for d in (2, 1, 3):
            along_v(ref, ref, 2, h, q, d)

    def spread_u(q, h):
        phase(f"mg1w{q}{h}")
        received(mb.at[0, 0, 0, pl.ds(0, 3)], rs_r.at[h, q, 2])
        ref = mb.at[h, q, rows_of[h][0]]
        for d in (2, 1, 3) if h else (2, 1, 3, 0):
            to = plane(tm, 0, d) if h else plane(tm - 1, d, 0)
            remote(ref, ref, rs_s.at[3 + (1 - h)], rs_r.at[h, q, 3], to).start()

    def second(q, k):
        mid = mb[c, q, :, :, k].astype(F32).reshape(128, 256).astype(BF16)
        return lax.dot_general(
            spec[q * 4 + k], mid, (((0,), (0,)), ((), ())), preferred_element_type=F32
        ).reshape(4, 64, 256)

    def pass_partials(q, k):
        at = pl.ds(k * 4, 4)
        return remote(ysend.at[q, at], yrecv.at[q, at], ys.at[0], yd_r.at[q], partner)

    def pass_local(q):
        return remote(ysend.at[q, z], yloc.at[q], ys.at[1], yl_r.at[q], partner)

    def sum_steps(q, direction):
        return 8 if (q < 2) == (direction == UP) else 7

    def sum_hop(q, distance):
        return SUM_HOPS[q // 2][distance]

    def sources(q, direction, left):
        return [d for d in range(8, 0, -1) if d <= sum_steps(q, direction) and d - sum_hop(q, d) == left]

    def ready(q, direction, left):
        after = [ready(q, direction, d) + 1.75 + 0.7 * sum_hop(q, d) for d in sources(q, direction, left)]
        return max(after, default=0.0)

    def ring_sum(q, direction, distance):
        hop = sum_hop(q, distance)
        sign = 1 if direction == UP else -1
        return remote(
            zsend.at[q, direction, distance - 1],
            zrecv.at[q, direction, distance - 1],
            zr_s.at[q],
            zr_r.at[q, direction, distance - 1],
            at_z(sign * hop, 0 if hop == distance and q < 2 else 1),
        )

    def ring_arrived(q, direction, left, value):
        for d in sources(q, direction, left):
            ring_sum(q, direction, d).wait_recv()
            value = value + zrecv[q, direction, d - 1].astype(F32)
        return value

    def finish(q, local):
        total = ring_arrived(q, DOWN, 0, ring_arrived(q, UP, 0, local))
        out_ref[:, q % 2, :] = x_ref[...].reshape(64, 256).astype(F32) + DAMP * total

    def events():
        listed = []
        for q in range(4):
            for h in range(2):
                late = 1.4 * q + 0.2 * (1 - h)
                for at, act in ((4.0, sum_u), (6.9, sum_v), (9.8, spread_u)):
                    listed.append((at + late, act, q, (h,)))
        return listed

    @pl.when(c == 1)
    def _():
        def multiply(q):
            phase(f"mg2w{q}")
            received(mb.at[1, q, pl.ds(0, 3)], rs_r.at[1, q, 3])
            phase(f"mg2c{q}")
            for k in range(4):
                part = second(q, k)
                yo[q, k * 4 : k * 4 + 4] = part
            if q < 2:
                ysend[q, z] = yo[q, z].astype(BF16)
                pass_local(q).start()

        def take_partials(q):
            phase(f"yw{q}")
            received(yrecv.at[q], yd_r.at[q])

        def ring_step(q, direction, distance):
            phase(f"zr{distance}{q}")
            sign = 1 if direction == UP else -1
            d = (z + sign * distance + NZ) % NZ
            value = ring_arrived(q, direction, distance, yo[q, d] + yrecv[q, d].astype(F32))
            zsend[q, direction, distance - 1] = value.astype(BF16)
            ring_sum(q, direction, distance).start()

        listed = events()
        for q in range(4):
            late = 1.4 * q
            listed.append((13.8 + late, multiply, q, ()))
            listed.append((15.8 + late, take_partials, q, ()))
            for distance in range(8, 0, -1):
                for direction in (UP, DOWN):
                    if distance <= sum_steps(q, direction):
                        at = 15.8 + late + ready(q, direction, distance)
                        listed.append((at, ring_step, q, (direction, distance)))
        for _, act, q, more in sorted(listed, key=lambda item: item[0]):
            act(q, *more)
        for q in (2, 3):
            phase(f"fin{q}")
            finish(q, yo[q, z] + yrecv[q, z].astype(F32))
        phase("sendw2")
        for q in range(4):
            sent(ysend.at[0, pl.ds(0, 15)], zr_s.at[q])
        sent(yloc, ys.at[1])
        for i, ref in enumerate((fs.at[pl.ds(0, 3)], f2r, f2r, fs.at[pl.ds(0, 3)], fs)):
            sent(ref, rs_s.at[i])

    @pl.when(c == 0)
    def _():
        def multiply(q):
            phase(f"mg2w{q}")
            received(mb.at[0, q], rs_r.at[0, q, 3])
            phase(f"mg2c{q}")
            for k in range(4):
                ysend[q, k * 4 : k * 4 + 4] = second(q, k).astype(BF16)
                pass_partials(q, k).start()

        for q in range(4):
            multiply(q)
        for q in (0, 1):
            phase(f"fin{q}")
            pass_local(q).wait_recv()
            finish(q, ysend[q, z].astype(F32) + yloc[q].astype(F32))
        phase("sendw2")
        sent(ysend, ys.at[0])
        sent(fs, rs_s.at[0])

    phase(None)


def shards(occ_orbitals, empty_orbitals, occ_rate, empty_rate, columns):
    vmem = pl.BlockSpec(memory_space=pltpu.VMEM)
    dma = pltpu.SemaphoreType.DMA

    out = pl.pallas_call(
        kernel,
        out_shape=jax.ShapeDtypeStruct((64, 2, 256), F32),
        in_specs=[pl.BlockSpec(memory_space=pltpu.HBM)] * 6,
        out_specs=vmem,
        scratch_shapes=[
            pltpu.VMEM((8, 8, 256), BF16),
            pltpu.VMEM((16, 128), F32),
            pltpu.VMEM((16, 128), F32),
            pltpu.VMEM((256, 256), BF16),
            pltpu.VMEM((16, 34, 8, 256), BF16),
            pltpu.VMEM((2, 4, 4, 8, 2, 8, 256), BF16),
            pltpu.VMEM((2, 2, 8, 256), BF16),
            pltpu.VMEM((2, 2048, 1024), BF16),
            pltpu.VMEM((2, 2048, 256), F32),
            pltpu.VMEM((16, 128, 256), BF16),
            pltpu.VMEM((16, 128, 256), BF16),
            pltpu.VMEM((256, 256), BF16),
            pltpu.VMEM((4, 4, 4, 4, 8, 256), BF16),
            pltpu.VMEM((2, 4, 4, 4, 4, 8, 256), BF16),
            pltpu.VMEM((2, 4, 4, 4, 8, 256), BF16),
            pltpu.VMEM((2, 4, 3, 4, 8, 256), BF16),
            pltpu.VMEM((2, 4, 4, 4, 4, 8, 256), BF16),
            pltpu.VMEM((4, 16, 64, 256), F32),
            pltpu.VMEM((4, 16, 64, 256), BF16),
            pltpu.VMEM((4, 16, 64, 256), BF16),
            pltpu.VMEM((2, 64, 256), BF16),
            pltpu.VMEM((4, 2, 8, 64, 256), BF16),
            pltpu.VMEM((4, 2, 8, 64, 256), BF16),
            dma((6,)),
            dma((2, 8, 4)),
            dma((2,)),
            dma((3,)),
            dma(()),
            dma((4,)),
            dma((4,)),
            dma(()),
            dma((7,)),
            dma((2, 4, 4)), dma((5,)),
            dma((4,)), dma((2,)), dma((2,)),
            dma((4, 2, 8)), dma((4,)),
        ],
        compiler_params=pltpu.CompilerParams(
            collective_id=0, has_side_effects=True, vmem_limit_bytes=48 * 1024 * 1024
        ),
        name="screen",
    )(
        *(
            pltpu.with_memory_space_constraint(a, pltpu.HBM)
            for a in (
                occ_orbitals.reshape(8, 8, 256),
                empty_orbitals.reshape(8, 8, 256),
                columns.reshape(8, 8, 256),
                occ_rate.reshape(16, 128),
                empty_rate.reshape(16, 128),
                transform_matrix(),
            )
        )
    )
    return out


def solution(mesh):
    placed = (P(("col", "row"), "tm"), P(("col", "row"), "tm"), P(), P(), P(("col", "row"), None))
    return jax.shard_map(
        shards, mesh=mesh, in_specs=placed, out_specs=P(("col", "row"), "tm", None), check_vma=False
    )
```

```python
import jax
import jax.numpy as jnp
import numpy as np
from jax import lax
from jax.experimental import pallas as pl
from jax.experimental.pallas import tpu as pltpu
from jax.sharding import PartitionSpec as P

MESH = pl.DeviceIdType.MESH
F32 = jnp.float32
BF16 = jnp.bfloat16
NT = 16
NZ = 16
DAMP = 0.3
PIECES = ((0, 10), (10, 8), (18, 8), (26, 8))
OFFSET = ((18, 26), (0, 10))
UP, DOWN = 0, 1
HOPS = (0, 1, 1, 1, 1, 1, 1, 1, 2)
EVEN = (0, 1, 2, 1, 2, 1, 2, 1, 2)
SUM_HOPS = ((0, 1, 2, 1, 2, 1, 1, 1, 1), (0, 1, 2, 1, 2, 1, 1, 1, 2), EVEN, EVEN)


_open = []


def phase(name):
    pass


def transform_matrix():
    moments = (0.25 * (np.arange(NT) + 0.5)).astype(np.float32)
    omegas = (0.4 * (np.arange(NT) + 0.5)).astype(np.float32)
    cosine = (0.5 * np.cos(omegas[:, None] * moments[None, :])).astype(np.float32)
    order = np.array([4 * zh + 2 * c + e for c in range(2) for e in range(2) for zh in range(4)])
    return jnp.asarray(np.kron(cosine[order], np.eye(16)), dtype=BF16)


def kernel(
    occ_in, emp_in, x_in, orate_in, erate_in, kron_in, out_ref,
    x_ref, orate_ref, erate_ref, kron_ref,
    colbuf, rowbuf, pk, lhs, acc, pol, spec, xc, fs, f1r, f1s, f2r, mb, yo, ysend, yrecv, yloc, zsend, zrecv,
    in_s, zag_r, zd_r, zo_r, r1_r, ag1_r, ag2_r, rd_r, gs, rs_r, rs_s, yd_r, yl_r, ys, zr_r, zr_s,
):
    tm, row, y = lax.axis_index("tm"), lax.axis_index("row"), lax.axis_index("col")
    c, zh = tm % 2, tm // 2
    zl, x = row // 4, row % 4
    z = zh * 4 + zl
    u = x * (1 - c) + y * c
    v = y * (1 - c) + x * c

    def at_z(step, core):
        other = (z + step + NZ) % NZ
        return ((other // 4) * 2 + core, (other % 4) * 4 + x, y)

    def plane(t, dx, dy):
        return (t, zl * 4 + (x + dx) % 4, (y + dy) % 4)

    def u_peer(d):
        return plane(tm, d * (1 - c), d * c)

    def v_peer(d):
        return plane(tm, d * c, d * (1 - c))

    partner = (zh * 2 + 1 - c, row, y)

    def remote(src, dst, ss, rs, dev):
        return pltpu.make_async_remote_copy(
            src_ref=src, dst_ref=dst, send_sem=ss, recv_sem=rs, device_id=dev, device_id_type=MESH
        )

    rows_of = [(x, y), (y, x)]
    far = (zh + 2) % 4
    late = [
        pltpu.make_async_copy(src, dst, in_s.at[i])
        for i, (src, dst) in enumerate(
            ((x_in, x_ref), (orate_in, orate_ref), (erate_in, erate_ref), (kron_in, kron_ref))
        )
    ]
    early = []
    for s, src in enumerate((occ_in, emp_in)):
        early.append((src, colbuf.at[z, pl.ds(OFFSET[0][s] * (1 - c) + OFFSET[1][s] * c, 8)]))
        for h in range(2):
            early.append((src.at[far * 2 + h], pk.at[h, s]))
            early.append((src.at[zh * 2 + h], rowbuf.at[h, rows_of[h][0], rows_of[h][1], tm, s]))
    early = [pltpu.make_async_copy(src, dst, in_s.at[4]) for src, dst in early]
    own_x = pltpu.make_async_copy(x_in.at[pl.ds(zh * 2, 2)], colbuf.at[z, pl.ds(8, 2)], in_s.at[5])
    for copy in early:
        copy.start()

    @pl.when(c == 1)
    def _():
        own_x.start()

    for copy in late:
        copy.start()

    phase("bar")
    barrier = pltpu.get_barrier_semaphore()
    peers = [partner, (far * 2, row, y), (far * 2 + 1, row, y)]
    peers += [at_z(step, core) for step in (1, -1, 2, -2) for core in (0, 1)]
    peers += [u_peer(d) for d in range(1, 4)] + [v_peer(d) for d in range(1, 4)]
    peers += [plane(tm + 1 - 2 * c, 0, d) for d in range(1, 4)]
    peers += [plane(tm + 1 - 2 * c, d, 0) for d in range(1, 4)]
    for peer in peers:
        pl.semaphore_signal(barrier, inc=1, device_id=peer, device_id_type=MESH)
    everything = ysend.at[0, pl.ds(0, 3)]
    pltpu.make_async_copy(everything, everything, in_s.at[4]).wait()

    @pl.when(c == 1)
    def _():
        own_x.wait()

    pl.semaphore_wait(barrier, len(peers))

    def received(ref, sem):
        remote(ref, ref, gs.at[0], sem, partner).wait_recv()

    def sent(ref, sem):
        remote(ref, ref, sem, zo_r.at[0], partner).wait_send()

    def to_row_gatherer(h):
        slot = rowbuf.at[h, rows_of[h][0], rows_of[h][1], tm]
        return remote(pk.at[h], slot, gs.at[0], r1_r, (far * 2, row, y))

    def steps(piece, direction):
        return 8 if (piece < 2) == (direction == UP) else 7

    def shard(owner, start, size):
        return colbuf.at[owner, pl.ds(start, size)]

    def ring_copy(direction, distance, piece):
        hop = HOPS[distance]
        sign = 1 if direction == UP else -1
        ref = shard((z - sign * (distance - hop) + NZ) % NZ, *PIECES[piece])
        return remote(ref, ref, gs.at[1], zag_r.at[direction, distance - 1, piece], at_z(sign * hop, 1))

    def pass_on(direction, reached, piece):
        for distance in (reached + 2, reached + 1):
            if distance <= steps(piece, direction) and HOPS[distance] == distance - reached:
                ring_copy(direction, distance, piece).start()

    def hand_over(direction, t, piece):
        ref = shard((z - 1 - t + NZ) % NZ if direction == UP else (z + 1 + t) % NZ, *PIECES[piece])
        return remote(ref, ref, gs.at[2], zd_r.at[t // 4], partner)

    def own_over(start, size, i):
        ref = shard(z, start, size)
        return remote(ref, ref, gs.at[3], zo_r.at[i], partner)

    def rows_over(block):
        ref = rowbuf.at[1, y, :, pl.ds(block * 2, 2)]
        return remote(ref, ref, gs.at[4], rd_r, partner)

    acc[...] = jnp.zeros_like(acc)

    @pl.when(c == 1)
    def _():
        phase("issue")
        for h in range(2):
            to_row_gatherer(h).start()
        for piece in range(2):
            for direction in (UP, DOWN):
                pass_on(direction, 0, piece)
        own_over(0, 18, 0).start()
        for piece in range(2, 4):
            own_over(*PIECES[piece], piece - 1).wait_recv()
            for direction in (UP, DOWN):
                pass_on(direction, 0, piece)
        for t in range(8):
            phase(f"z{t}")
            for piece in range(4):
                for direction in (UP, DOWN):
                    if t >= steps(piece, direction):
                        continue
                    ring_copy(direction, t + 1, piece).wait_recv()
                    pass_on(direction, t + 1, piece)
                    hand_over(direction, t, piece).start()
        phase("roww")
        received(rowbuf.at[1], rd_r)
        phase("sendw")
        sent(pk, gs.at[0])
        sent(colbuf.at[pl.ds(0, 15)], gs.at[1])
        sent(colbuf.at[pl.ds(0, 15)], gs.at[2])
        sent(colbuf.at[0, pl.ds(0, 18)], gs.at[3])

    @pl.when(c == 0)
    def _():
        phase("issue")
        for piece in range(2, 4):
            own_over(*PIECES[piece], piece - 1).start()
        for h in range(2):
            to_row_gatherer(h).start()

        def take_rows(owner, source):
            for s in range(2):
                for h in range(2):
                    slot = (h, rows_of[h][0], rows_of[h][1], (owner // 4) * 2 + source, s)
                    rowbuf[slot] = colbuf[owner, OFFSET[source][s] + zh * 2 + h]

        def first_stage(k):
            for d in (2, 1, 3):
                for h in range(2):
                    ref = rowbuf.at[h, rows_of[h][0], rows_of[h][1], pl.ds(((zh + k) % 4) * 2, 2)]
                    remote(ref, ref, gs.at[5], ag1_r.at[k], plane(tm, d * h, d * (1 - h))).start()

        def second_stage(k):
            phase(f"ag1w{k}")
            received(ysend.at[0, pl.ds(0, 3)], ag1_r.at[k])
            for back in range(4):
                for d in (2, 1, 3):
                    for h in range(2):
                        uo, vo = (x, (y - back + 4) % 4) if h == 0 else (y, (x - back + 4) % 4)
                        ref = rowbuf.at[h, uo, vo, pl.ds(((zh + k) % 4) * 2, 2)]
                        arrived = rd_r if h else ag2_r.at[k]
                        remote(ref, ref, gs.at[6], arrived, plane(tm + h, d * (1 - h), d * h)).start()
            rows_over((zh + k) % 4).start()

        def third_stage(k):
            phase(f"ag2w{k}")
            received(ysend.at[0, pl.ds(0, 6)], ag2_r.at[k])

        own_over(0, 18, 0).wait_recv()
        take_rows(z, 1)
        first_stage(0)
        second_stage(0)
        phase("r1w")
        received(ysend.at[0, 0], r1_r)
        first_stage(2)
        third_stage(0)
        second_stage(2)
        phase("z3w")
        received(colbuf.at[pl.ds(0, 8)], zd_r.at[0])
        for k in (1, 3):
            for source in range(2):
                take_rows((z + 4 * k) % NZ, source)
            first_stage(k)
        third_stage(2)
        for k in (1, 3):
            second_stage(k)
        for k in (1, 3):
            third_stage(k)
        phase("colw")
        received(colbuf.at[pl.ds(0, 7)], zd_r.at[1])
        phase("sendw")
        sent(pk, gs.at[0])
        sent(colbuf.at[0, pl.ds(0, 16)], gs.at[3])
        sent(rowbuf.at[1, 0], gs.at[4])
        sent(ysend.at[0, pl.ds(0, 12)], gs.at[5])
        sent(ysend.at[pl.ds(0, 3)], gs.at[6])

    phase("green")
    for copy in late:
        copy.wait()
    moments = 0.25 * (lax.broadcasted_iota(jnp.int32, (NT, 128), 0).astype(F32) + 0.5)

    @pl.loop(0, 2)
    def _(b):
        for s, rate_ref in ((0, orate_ref), (1, erate_ref)):
            cols = []
            for k in range(4):
                at = (b * 4 + k) * 2
                weights = jnp.concatenate(
                    [jnp.exp(-rate_ref[pl.ds(at + i, 1), :] * moments) for i in range(2)], axis=1
                )
                rows = rowbuf[c, :, :, b * 4 + k, s].astype(F32).reshape(128, 256)
                for j in range(NT):
                    lhs[s, j * 128 : (j + 1) * 128, k * 256 : (k + 1) * 256] = (
                        rows * weights[j : j + 1, :]
                    ).astype(BF16)
                first = OFFSET[k % 2][s]
                cols.append(colbuf[pl.ds(b * 8 + k // 2 * 4, 4), first : first + 8].reshape(256, 256))
            acc[s] += lax.dot_general(
                lhs[s], jnp.concatenate(cols, axis=1), (((1,), (1,)), ((), ())), preferred_element_type=F32
            )

    phase("pol")
    for j in range(NT):
        at = pl.ds(j * 128, 128)
        pol[j] = (-2.0 * acc[0, at, :] * acc[1, at, :]).astype(BF16)
    phase("trans")
    for g in range(8):
        at = slice(g * 16, g * 16 + 16)
        mixed = jnp.dot(kron_ref[...], pol[:, at, :].reshape(256, 256), preferred_element_type=F32)
        spec[:, at, :] = mixed.astype(BF16).reshape(16, 16, 256)
    for h in range(4):
        for i in range(4):
            xc[i * 64 + h * 16 : i * 64 + h * 16 + 16, :] = colbuf[h * 4 + i, 8:10].reshape(16, 256)

    def to_sum_u(q, d):
        to = plane(zh * 2 + 1, d * (1 - c), d * c)
        return remote(fs.at[q, (u + d) % 4], f1r.at[c, q, d], rs_s.at[0], rs_r.at[c, q, 0], to)

    def along_v(src, dst, stage, h, q, d):
        plane_v = plane(tm, d * h, d * (1 - h))
        remote(src, dst, rs_s.at[stage], rs_r.at[h, q, stage], plane_v).start()

    for q in range(4):
        phase(f"first{q}")
        for k in range(4):
            part = jnp.dot(spec[q * 4 + k], xc[...], preferred_element_type=F32)
            fs[q, :, :, k] = part.reshape(4, 4, 8, 256).astype(BF16)
        for d in (2, 1, 3):
            to_sum_u(q, d).start()

        @pl.when(c == 0)
        def _(q=q):
            to_sum_u(q, 0).start()

    def sum_u(q, h):
        phase(f"rs1w{q}{h}")
        received(f1r.at[1, q, pl.ds(1, 3)] if h else f1r.at[0, q], rs_r.at[h, q, 0])
        total = (fs[q, u] if h else f1r[0, q, 0]).astype(F32)
        for d in range(1, 4):
            total = total + f1r[h, q, d].astype(F32)
        f1s[h, q] = total.astype(BF16)
        for d in (2, 1, 3):
            along_v(f1s.at[h, q, (rows_of[h][1] + d) % 4], f2r.at[h, q, d - 1], 1, h, q, d)

    def sum_v(q, h):
        phase(f"rs2w{q}{h}")
        received(f2r.at[h, q], rs_r.at[h, q, 1])
        total = f1s[h, q, rows_of[h][1]].astype(F32)
        for d in range(3):
            total = total + f2r[h, q, d].astype(F32)
        mb[h, q, rows_of[h][0], rows_of[h][1]] = (
            x_ref[zh * 2 + h].astype(F32)[None] + DAMP * total
        ).astype(BF16)
        ref = mb.at[h, q, rows_of[h][0], rows_of[h][1]]
        for d in (2, 1, 3):
            along_v(ref, ref, 2, h, q, d)

    def spread_u(q, h):
        phase(f"mg1w{q}{h}")
        received(mb.at[0, 0, 0, pl.ds(0, 3)], rs_r.at[h, q, 2])
        ref = mb.at[h, q, rows_of[h][0]]
        for d in (2, 1, 3) if h else (2, 1, 3, 0):
            to = plane(tm, 0, d) if h else plane(tm - 1, d, 0)
            remote(ref, ref, rs_s.at[3 + (1 - h)], rs_r.at[h, q, 3], to).start()

    def second(q, k):
        mid = mb[c, q, :, :, k].astype(F32).reshape(128, 256).astype(BF16)
        return lax.dot_general(
            spec[q * 4 + k], mid, (((0,), (0,)), ((), ())), preferred_element_type=F32
        ).reshape(4, 64, 256)

    def pass_partials(q, k):
        at = pl.ds(k * 4, 4)
        return remote(ysend.at[q, at], yrecv.at[q, at], ys.at[0], yd_r.at[q], partner)

    def pass_local(q):
        return remote(ysend.at[q, z], yloc.at[q], ys.at[1], yl_r.at[q], partner)

    def sum_steps(q, direction):
        return 8 if (q < 2) == (direction == UP) else 7

    def sum_hop(q, distance):
        return SUM_HOPS[q][distance]

    def sources(q, direction, left):
        return [d for d in range(8, 0, -1) if d <= sum_steps(q, direction) and d - sum_hop(q, d) == left]

    def ready(q, direction, left):
        after = [ready(q, direction, d) + 1.75 + 0.7 * sum_hop(q, d) for d in sources(q, direction, left)]
        return max(after, default=0.0)

    def ring_sum(q, direction, distance):
        hop = sum_hop(q, distance)
        sign = 1 if direction == UP else -1
        return remote(
            zsend.at[q, direction, distance - 1],
            zrecv.at[q, direction, distance - 1],
            zr_s.at[q],
            zr_r.at[q, direction, distance - 1],
            at_z(sign * hop, 0 if hop == distance and q < 2 else 1),
        )

    def ring_arrived(q, direction, left, value):
        for d in sources(q, direction, left):
            ring_sum(q, direction, d).wait_recv()
            value = value + zrecv[q, direction, d - 1].astype(F32)
        return value

    def finish(q, local):
        total = ring_arrived(q, DOWN, 0, ring_arrived(q, UP, 0, local))
        out_ref[:, q % 2, :] = x_ref[...].reshape(64, 256).astype(F32) + DAMP * total

    def events():
        listed = []
        for q in range(4):
            for h in range(2):
                late = 1.4 * q + 0.2 * (1 - h)
                for at, act in ((4.0, sum_u), (6.9, sum_v), (9.8, spread_u)):
                    listed.append((at + late, act, q, (h,)))
        return listed

    @pl.when(c == 1)
    def _():
        def multiply(q):
            phase(f"mg2w{q}")
            received(mb.at[1, q, pl.ds(0, 3)], rs_r.at[1, q, 3])
            phase(f"mg2c{q}")
            for k in range(4):
                part = second(q, k)
                yo[q, k * 4 : k * 4 + 4] = part
            if q < 2:
                ysend[q, z] = yo[q, z].astype(BF16)
                pass_local(q).start()

        def take_partials(q):
            phase(f"yw{q}")
            received(yrecv.at[q], yd_r.at[q])

        def ring_step(q, direction, distance):
            phase(f"zr{distance}{q}")
            sign = 1 if direction == UP else -1
            d = (z + sign * distance + NZ) % NZ
            value = ring_arrived(q, direction, distance, yo[q, d] + yrecv[q, d].astype(F32))
            zsend[q, direction, distance - 1] = value.astype(BF16)
            ring_sum(q, direction, distance).start()

        listed = events()
        for q in range(4):
            late = 1.4 * q
            listed.append((13.8 + late, multiply, q, ()))
            listed.append((15.8 + late, take_partials, q, ()))
            for distance in range(8, 0, -1):
                for direction in (UP, DOWN):
                    if distance <= sum_steps(q, direction):
                        at = 15.8 + late + ready(q, direction, distance)
                        listed.append((at, ring_step, q, (direction, distance)))
        for _, act, q, more in sorted(listed, key=lambda item: item[0]):
            act(q, *more)
        for q in (2, 3):
            phase(f"fin{q}")
            finish(q, yo[q, z] + yrecv[q, z].astype(F32))
        phase("sendw2")
        for q in range(4):
            sent(ysend.at[0, pl.ds(0, 15)], zr_s.at[q])
        sent(yloc, ys.at[1])
        for i, ref in enumerate((fs.at[pl.ds(0, 3)], f2r, f2r, fs.at[pl.ds(0, 3)], fs)):
            sent(ref, rs_s.at[i])

    @pl.when(c == 0)
    def _():
        def multiply(q):
            phase(f"mg2w{q}")
            received(mb.at[0, q], rs_r.at[0, q, 3])
            phase(f"mg2c{q}")
            for k in range(4):
                ysend[q, k * 4 : k * 4 + 4] = second(q, k).astype(BF16)
                pass_partials(q, k).start()

        for q in range(4):
            multiply(q)
        for q in (0, 1):
            phase(f"fin{q}")
            pass_local(q).wait_recv()
            finish(q, ysend[q, z].astype(F32) + yloc[q].astype(F32))
        phase("sendw2")
        sent(ysend, ys.at[0])
        sent(fs, rs_s.at[0])

    phase(None)


def shards(occ_orbitals, empty_orbitals, occ_rate, empty_rate, columns):
    vmem = pl.BlockSpec(memory_space=pltpu.VMEM)
    dma = pltpu.SemaphoreType.DMA

    out = pl.pallas_call(
        kernel,
        out_shape=jax.ShapeDtypeStruct((64, 2, 256), F32),
        in_specs=[pl.BlockSpec(memory_space=pltpu.HBM)] * 6,
        out_specs=vmem,
        scratch_shapes=[
            pltpu.VMEM((8, 8, 256), BF16),
            pltpu.VMEM((16, 128), F32),
            pltpu.VMEM((16, 128), F32),
            pltpu.VMEM((256, 256), BF16),
            pltpu.VMEM((16, 34, 8, 256), BF16),
            pltpu.VMEM((2, 4, 4, 8, 2, 8, 256), BF16),
            pltpu.VMEM((2, 2, 8, 256), BF16),
            pltpu.VMEM((2, 2048, 1024), BF16),
            pltpu.VMEM((2, 2048, 256), F32),
            pltpu.VMEM((16, 128, 256), BF16),
            pltpu.VMEM((16, 128, 256), BF16),
            pltpu.VMEM((256, 256), BF16),
            pltpu.VMEM((4, 4, 4, 4, 8, 256), BF16),
            pltpu.VMEM((2, 4, 4, 4, 4, 8, 256), BF16),
            pltpu.VMEM((2, 4, 4, 4, 8, 256), BF16),
            pltpu.VMEM((2, 4, 3, 4, 8, 256), BF16),
            pltpu.VMEM((2, 4, 4, 4, 4, 8, 256), BF16),
            pltpu.VMEM((4, 16, 64, 256), F32),
            pltpu.VMEM((4, 16, 64, 256), BF16),
            pltpu.VMEM((4, 16, 64, 256), BF16),
            pltpu.VMEM((2, 64, 256), BF16),
            pltpu.VMEM((4, 2, 8, 64, 256), BF16),
            pltpu.VMEM((4, 2, 8, 64, 256), BF16),
            dma((6,)),
            dma((2, 8, 4)),
            dma((2,)),
            dma((3,)),
            dma(()),
            dma((4,)),
            dma((4,)),
            dma(()),
            dma((7,)),
            dma((2, 4, 4)), dma((5,)),
            dma((4,)), dma((2,)), dma((2,)),
            dma((4, 2, 8)), dma((4,)),
        ],
        compiler_params=pltpu.CompilerParams(
            collective_id=0, has_side_effects=True, vmem_limit_bytes=48 * 1024 * 1024
        ),
        name="screen",
    )(
        *(
            pltpu.with_memory_space_constraint(a, pltpu.HBM)
            for a in (
                occ_orbitals.reshape(8, 8, 256),
                empty_orbitals.reshape(8, 8, 256),
                columns.reshape(8, 8, 256),
                occ_rate.reshape(16, 128),
                empty_rate.reshape(16, 128),
                transform_matrix(),
            )
        )
    )
    return out


def solution(mesh):
    placed = (P(("col", "row"), "tm"), P(("col", "row"), "tm"), P(), P(), P(("col", "row"), None))
    return jax.shard_map(
        shards, mesh=mesh, in_specs=placed, out_specs=P(("col", "row"), "tm", None), check_vma=False
    )
```
